32 devices in a mesh: grp: 2 (over x), seq: 16 (over z, y, core).
Axes of the slice: x: 2, y: 2, z: 4, core: 2. Of those that a mesh axis runs over, the one named last changes fastest.
Arguments:
- llm_grad: bfloat16 [4096, 8192], P('seq', 'grp'), may hold values from -6 to 6
- image_grid: int32 [256, 2], replicated, may hold values from 1 to 3, as said below
- image_owner: int32 [256], replicated, may hold values from 0 to 15, as said below
- row_start: int32 [256], replicated, may hold values from 0 to 255, as said below
- merger_pre: bfloat16 [48, 16, 2560], P(None, 'seq', 'grp'), may hold values from -6 to 6
- vit_out: bfloat16 [192, 16, 1280], P(None, 'seq'), may hold values from -6 to 6
- vit_pre: bfloat16 [192, 16, 2560], P(None, 'seq', 'grp'), may hold values from -6 to 6
- ln_gain: float32 [1280], replicated, may hold values from 0.25 to 1.75
- merger_out_w: bfloat16 [8192, 2560], P('seq', 'grp'), may hold values from -0.0625 to 0.0625
- merger_in_w: bfloat16 [2560, 5120], P('grp', 'seq'), may hold values from -0.125 to 0.125
- vit_fc2_w: bfloat16 [1280, 2560], P('seq', 'grp'), may hold values from -0.15625 to 0.15625
Outputs:
- patch_grad: bfloat16 [192, 16, 1280], P('grp', 'seq')
- fc1_grad: bfloat16 [192, 16, 2560], P(None, 'seq', 'grp')
- fc2_w_grad: float32 [1280, 2560], P('seq', 'grp')
The draws below stay inside these ranges and needn't reach their ends.
Inputs may be any that keep to these rules, and one draw needn't show every extreme that they name: `image_grid`: height times width is 1 to 3; the first image of every shard is 1 by 3; the last image of shard 0 is 1 by 1. `image_owner`: the 16 images of one shard have 16 different owners. An image's rows row_start to row_start + t - 1 lie inside its shard and meet no other image's rows; a shard's images follow the order of k; the last image of every shard ends at the shard's last row; the first image of shard 0 starts at row 0.
All inputs are finite; a program needn't handle non-finite values.
Results may differ from the reference program's by a relative error of at most 0.02.
Values may be sent and summed in bfloat16 or wider, within the bound.
A program may use at most 128 MiB of HBM per device.

```python
import jax
import jax.numpy as jnp
from jax import lax

D_LLM = 8192
VIT = 1280
HID = 2560
VHID = 2560
SLOT = 3
SEQ_TOK = 256
MERGE_IN = 5120
IMAGES = 256
MROWS = 48
PSLOT = 192
LLM_TOK = 4096
N_GRP = 2
N_SEQ = 16


def image_layout(key):
    shape_ids = jax.random.randint(jax.random.fold_in(key, 101), (N_SEQ, N_SEQ), 0, 5)
    shape_ids = shape_ids.at[:, 0].set(3)
    shape_ids = shape_ids.at[0, N_SEQ - 1].set(0)
    heights = jnp.array([1, 1, 2, 1, 3], jnp.int32)[shape_ids]
    widths = jnp.array([1, 2, 1, 3, 1], jnp.int32)[shape_ids]
    owner_keys = jax.random.split(jax.random.fold_in(key, 202), N_SEQ)
    owners = jax.vmap(lambda one_key: jax.random.permutation(one_key, N_SEQ))(owner_keys).astype(jnp.int32)
    most_gap = (SEQ_TOK - SLOT * N_SEQ) // N_SEQ
    gap_rows = jax.random.randint(jax.random.fold_in(key, 303), (N_SEQ, N_SEQ), 0, most_gap + 1)
    gap_rows = gap_rows.at[0, 0].set(0)
    token_counts = heights * widths
    span_rows = gap_rows + token_counts
    starts = jnp.cumsum(span_rows, axis=1) - token_counts
    starts = starts.at[:, N_SEQ - 1].set(SEQ_TOK - token_counts[:, N_SEQ - 1])
    return (heights, widths, owners, starts.astype(jnp.int32))


def draw_image_grid(key, part):
    heights, widths, owners, starts = image_layout(key)
    return jnp.stack([heights, widths], -1).reshape(IMAGES, 2).astype(jnp.int32)


def draw_image_owner(key, part):
    heights, widths, owners, starts = image_layout(key)
    return owners.reshape(IMAGES)


def draw_row_start(key, part):
    heights, widths, owners, starts = image_layout(key)
    return starts.reshape(IMAGES)


def shard_levels(key, extent, cuts, least, largest):
    gain = 1.0
    for dim, shards_of in cuts:
        steps = jax.random.uniform(jax.random.fold_in(jax.random.fold_in(key, 6), dim), (shards_of,), jnp.float32, least / len(cuts), largest / len(cuts))
        gain = gain * jnp.repeat(jnp.exp(steps), extent[dim] // shards_of).reshape((-1,) + (1,) * (len(extent) - 1 - dim))
    return gain


def gaussian(own_key, shape, spread, reach, cuts=(), kind=jnp.bfloat16):
    entries = jax.random.normal(own_key, shape, jnp.float32) * spread
    if len(cuts) > 0:
        entries = shard_levels(own_key, shape, cuts, -0.22, 0.18) * entries
    return jnp.clip(entries, min=-reach, max=reach).astype(kind)


def setup_inputs(seed: int = 0) -> dict:
    seeds = jax.random.split(jax.random.key(seed), 12)
    return {
        "llm_grad": gaussian(seeds[0], (LLM_TOK, D_LLM), 1.0, 6.0, ((0, 16), (1, 2))),
        "image_grid": draw_image_grid(jax.random.fold_in(seeds[11], 71), 0),
        "image_owner": draw_image_owner(jax.random.fold_in(seeds[11], 71), 0),
        "row_start": draw_row_start(jax.random.fold_in(seeds[11], 71), 0),
        "merger_pre": gaussian(seeds[4], (MROWS, N_SEQ, HID), 1.0, 6.0, ((1, 16), (2, 2))),
        "vit_out": gaussian(seeds[5], (PSLOT, N_SEQ, VIT), 1.0, 6.0, ((1, 16),)),
        "vit_pre": gaussian(seeds[6], (PSLOT, N_SEQ, VHID), 1.0, 6.0, ((1, 16), (2, 2))),
        "ln_gain": jnp.clip(1.0 + 0.15 * jax.random.normal(seeds[7], (VIT,), jnp.float32), 0.25, 1.75),
        "merger_out_w": gaussian(seeds[8], (D_LLM, HID), D_LLM ** -0.5, 0.0625, ((0, 16), (1, 2))),
        "merger_in_w": gaussian(seeds[9], (HID, MERGE_IN), HID ** -0.5, 0.125, ((0, 2), (1, 16))),
        "vit_fc2_w": gaussian(seeds[10], (VIT, VHID), VIT ** -0.5, 0.15625, ((0, 16), (1, 2))),
    }


def gelu_slope(values):
    return 0.5 * (1.0 + lax.erf(values * 0.7071067811865476)) + values * jnp.exp(-0.5 * values * values) * 0.3989422804014327

def patch_table(widths, counts, slots):
    places = jnp.arange(4 * slots, dtype=jnp.int32)
    merged = places // 4
    corner = places % 4
    row_in = merged[None, :] // widths[:, None]
    col_in = merged[None, :] % widths[:, None]
    target = (2 * row_in + corner[None, :] // 2) * (2 * widths[:, None]) + 2 * col_in + corner[None, :] % 2
    usable = merged[None, :] < counts[:, None]
    return ((target[:, None, :] == places[None, :, None]) & usable[:, None, :]).astype(jnp.float32)

def norm_backward(upstream, inputs, scales):
    average = lax.optimization_barrier(jnp.mean(inputs, -1, keepdims=True))
    centred = inputs - average
    inverse_std = lax.rsqrt(lax.optimization_barrier(jnp.mean(centred * centred, -1, keepdims=True)) + 1e-06)
    normed = centred * inverse_std
    scaled = upstream * scales
    return inverse_std * (scaled - lax.optimization_barrier(jnp.mean(scaled, -1, keepdims=True)) - normed * lax.optimization_barrier(jnp.mean(scaled * normed, -1, keepdims=True)))

def reference(llm_grad, image_grid, image_owner, row_start, merger_pre, vit_out, vit_pre, ln_gain, merger_out_w, merger_in_w, vit_fc2_w):
    grids = image_grid.reshape(N_SEQ, N_SEQ, 2)
    counts = grids[:, :, 0] * grids[:, :, 1]
    widths = grids[:, :, 1]
    owners = image_owner.reshape(N_SEQ, N_SEQ)
    starts = row_start.reshape(N_SEQ, N_SEQ)
    block_width = HID // N_GRP
    sources = jnp.arange(N_SEQ, dtype=jnp.int32)
    within = jnp.arange(SLOT, dtype=jnp.int32)
    in_blocks = merger_in_w.reshape(N_GRP, block_width, MERGE_IN).astype(jnp.float32)

    def one_owner(weight_grad, owner_id):
        chosen = (owners == owner_id).astype(jnp.int32)
        own_counts = lax.optimization_barrier(jnp.sum(chosen * counts, 1))
        own_widths = lax.optimization_barrier(jnp.sum(chosen * widths, 1))
        own_starts = lax.optimization_barrier(jnp.sum(chosen * starts, 1))
        indices = sources[:, None] * SEQ_TOK + jnp.minimum(own_starts[:, None] + within[None, :], SEQ_TOK - 1)
        usable = within[None, :] < own_counts[:, None]
        picked = jnp.take(llm_grad, indices.reshape(-1).astype(jnp.int32), axis=0)
        returned = jnp.where(usable.reshape(-1, 1), picked, jnp.zeros_like(picked))
        hidden_grad = jnp.dot(returned, merger_out_w, preferred_element_type=jnp.float32).astype(jnp.bfloat16)
        pre_act = merger_pre[:, owner_id, :].astype(jnp.float32)
        pre_grad = (gelu_slope(pre_act) * hidden_grad.astype(jnp.float32)).astype(jnp.bfloat16)
        partial_sums = jnp.einsum('rgh,ghc->grc', pre_grad.astype(jnp.float32).reshape(MROWS, N_GRP, block_width), in_blocks)
        rounded = lax.optimization_barrier(partial_sums.astype(jnp.bfloat16))
        merged_grad = lax.optimization_barrier(jnp.sum(rounded.astype(jnp.float32), 0))
        table = patch_table(own_widths, own_counts, SLOT)
        patch_in = jnp.einsum('spq,sqc->spc', table, merged_grad.reshape(N_SEQ, 4 * SLOT, VIT), precision=lax.Precision.HIGHEST).reshape(PSLOT, VIT)
        patch_grad = norm_backward(patch_in, vit_out[:, owner_id, :].astype(jnp.float32), ln_gain).astype(jnp.bfloat16)
        fc_in = vit_pre[:, owner_id, :].astype(jnp.float32)
        sigmoid_q = jax.nn.sigmoid(1.702 * fc_in)
        activation = (fc_in * sigmoid_q).astype(jnp.bfloat16)
        act_grad = jnp.dot(patch_grad, vit_fc2_w, preferred_element_type=jnp.float32)
        fc1_grad = ((sigmoid_q + 1.702 * fc_in * sigmoid_q * (1.0 - sigmoid_q)) * act_grad).astype(jnp.bfloat16)
        weight_grad = weight_grad + lax.dot_general(patch_grad, activation, (((0,), (0,)), ((), ())), preferred_element_type=jnp.float32)
        return (weight_grad, (patch_grad, fc1_grad))
    weight_grad, stacked = lax.scan(one_owner, jnp.zeros((VIT, VHID), jnp.float32), sources)
    return (jnp.transpose(stacked[0], (1, 0, 2)), jnp.transpose(stacked[1], (1, 0, 2)), weight_grad)
```

```python
import functools

import jax
import jax.numpy as jnp
from jax import lax
from jax.experimental import pallas as pl
from jax.experimental.pallas import tpu as pltpu
from jax.sharding import PartitionSpec as P

SLOT = 3
MESH = pl.DeviceIdType.MESH
F32 = jnp.float32
BF16 = jnp.bfloat16


def gelu_slope(values):
    return (
        0.5 * (1.0 + lax.erf(values * 0.7071067811865476))
        + values * jnp.exp(-0.5 * values * values) * 0.3989422804014327
    )


def patch_table(widths, counts, slots):
    places = jnp.arange(4 * slots, dtype=jnp.int32)
    merged = places // 4
    corner = places % 4
    row_in = merged[None, :] // widths[:, None]
    col_in = merged[None, :] % widths[:, None]
    target = (
        (2 * row_in + corner[None, :] // 2) * (2 * widths[:, None])
        + 2 * col_in
        + corner[None, :] % 2
    )
    usable = merged[None, :] < counts[:, None]
    return ((target[:, None, :] == places[None, :, None]) & usable[:, None, :]).astype(jnp.float32)


def norm_backward(upstream, inputs, scales):
    average = jnp.mean(inputs, -1, keepdims=True)
    centred = inputs - average
    inverse_std = lax.rsqrt(jnp.mean(centred * centred, -1, keepdims=True) + 1e-06)
    normed = centred * inverse_std
    scaled = upstream * scales
    return inverse_std * (
        scaled
        - jnp.mean(scaled, -1, keepdims=True)
        - normed * jnp.mean(scaled * normed, -1, keepdims=True)
    )


def on_device(
    llm_grad,
    image_grid,
    image_owner,
    row_start,
    merger_pre,
    vit_out,
    vit_pre,
    ln_gain,
    merger_out_w,
    merger_in_w,
    vit_fc2_w,
):
    seq_count = lax.axis_size("seq")
    own_index = lax.axis_index("seq")
    grids = image_grid.reshape(seq_count, seq_count, 2)
    counts = grids[:, :, 0] * grids[:, :, 1]
    widths = grids[:, :, 1]
    owners = image_owner.reshape(seq_count, seq_count)
    starts = row_start.reshape(seq_count, seq_count)
    within = jnp.arange(SLOT, dtype=jnp.int32)
    peers = jnp.arange(seq_count, dtype=jnp.int32)
    shard_rows = llm_grad.shape[0]
    my_owners = lax.dynamic_index_in_dim(owners, own_index, 0, keepdims=False)
    my_counts = lax.dynamic_index_in_dim(counts, own_index, 0, keepdims=False)
    my_starts = lax.dynamic_index_in_dim(starts, own_index, 0, keepdims=False)
    targets = (my_owners[None, :] == peers[:, None]).astype(jnp.int32)
    send_counts = jnp.sum(targets * my_counts[None, :], 1)
    send_starts = jnp.sum(targets * my_starts[None, :], 1)
    indices = jnp.minimum(send_starts[:, None] + within[None, :], shard_rows - 1)
    usable = within[None, :] < send_counts[:, None]
    picked = jnp.take(llm_grad, indices.reshape(-1), axis=0)
    outgoing = jnp.where(usable.reshape(-1, 1), picked, jnp.zeros_like(picked)).reshape(
        seq_count, SLOT, llm_grad.shape[1]
    )
    received = (owners == own_index).astype(jnp.int32)
    recv_counts = jnp.sum(received * counts, 1)
    recv_widths = jnp.sum(received * widths, 1)
    wide_rows = lax.all_gather(
        outgoing.reshape(-1, llm_grad.shape[1]), "grp", axis=1, tiled=True
    )
    sliced = lax.all_to_all(wide_rows, "seq", split_axis=1, concat_axis=0, tiled=True)
    features = sliced.shape[1]
    by_owner = jnp.swapaxes(
        sliced.reshape(seq_count, seq_count, SLOT, features), 0, 1
    ).reshape(-1, features)
    folded = jnp.dot(by_owner, merger_out_w, preferred_element_type=jnp.float32)
    arrived = lax.all_to_all(
        folded.astype(jnp.bfloat16), "seq", split_axis=0, concat_axis=0, tiled=True
    )
    unit_grad = jnp.sum(
        arrived.reshape(seq_count, seq_count * SLOT, -1).astype(jnp.float32), 0
    ).astype(jnp.bfloat16)
    pre_act = merger_pre[:, 0, :].astype(jnp.float32)
    pre_grad = (gelu_slope(pre_act) * unit_grad.astype(jnp.float32)).astype(jnp.bfloat16)
    all_pre = lax.all_gather(pre_grad, "seq", axis=0, tiled=True)
    part_cols = jnp.dot(all_pre, merger_in_w, preferred_element_type=jnp.float32)
    part_rows = lax.all_to_all(
        part_cols.astype(jnp.bfloat16), "seq", split_axis=0, concat_axis=1, tiled=True
    )
    merged_part = jnp.sum(
        lax.all_gather(part_rows, "grp", axis=0).astype(jnp.float32), 0
    )
    vit_width = vit_out.shape[2]
    table = patch_table(recv_widths, recv_counts, SLOT)
    patch_in = jnp.einsum(
        "spq,sqc->spc",
        table,
        merged_part.reshape(seq_count, 4 * SLOT, vit_width),
        precision=lax.Precision.HIGHEST,
    ).reshape(-1, vit_width)
    patch_grad = norm_backward(patch_in, vit_out[:, 0, :].astype(jnp.float32), ln_gain).astype(
        jnp.bfloat16
    )
    group_rows = patch_grad.shape[0] // lax.axis_size("grp")
    own_rows = lax.dynamic_slice_in_dim(
        patch_grad, lax.axis_index("grp") * group_rows, group_rows, 0
    )
    act_grad = jnp.dot(
        patch_grad,
        lax.all_gather(vit_fc2_w, "seq", axis=0, tiled=True),
        preferred_element_type=jnp.float32,
    )
    fc_in = vit_pre[:, 0, :].astype(jnp.float32)
    sigmoid_q = jax.nn.sigmoid(1.702 * fc_in)
    activation = (fc_in * sigmoid_q).astype(jnp.bfloat16)
    fc1_grad = ((sigmoid_q + 1.702 * fc_in * sigmoid_q * (1.0 - sigmoid_q)) * act_grad).astype(
        jnp.bfloat16
    )
    weight_part = lax.dot_general(
        patch_grad, activation, (((0,), (0,)), ((), ())), preferred_element_type=jnp.float32
    )
    weight_parts = lax.all_to_all(
        weight_part.astype(jnp.bfloat16), "seq", split_axis=0, concat_axis=0, tiled=True
    )
    weight_grad = jnp.sum(
        weight_parts.reshape(seq_count, -1, weight_part.shape[1]).astype(jnp.float32), 0
    )
    return (
        own_rows.reshape(group_rows, 1, vit_width),
        fc1_grad.reshape(-1, 1, vit_pre.shape[2]),
        weight_grad,
    )


def small_div(values, by):
    return (values * ((65536 + by - 1) // by)) >> 16


def iota(shape, dim):
    return lax.broadcasted_iota(jnp.int32, shape, dim)


def sum_where(mask, values):
    return jnp.sum(jnp.where(mask, values, 0.0), 1, keepdims=True).astype(jnp.int32)


def fused_kernel(
    n_grp,
    n_seq,
    llm,
    grid,
    owner,
    start,
    mpre,
    vout,
    vpre,
    gain,
    wout,
    win,
    fc2,
    pg_out,
    fc1_out,
    wg_out,
    llm_v,
    mpre_v,
    vout_v,
    vpre_v,
    wo,
    wi2,
    wi,
    wf,
    act,
    fslope,
    gslope,
    rows_all,
    xin,
    xflat,
    xperm,
    ys,
    own1,
    ry,
    zs,
    rz,
    allp,
    p2,
    xs,
    own2,
    rx,
    a2s,
    mg,
    m4,
    pgall,
    fc1_v,
    own3,
    y3s,
    ry3,
    z3s,
    rz3,
    wg_v,
    ld_sem,
    out_sem,
    send_sem,
    xw_sem,
    xag_sem,
    xin_sem,
    ry_sem,
    rz_sem,
    agz_sem,
    agy_sem,
    rx_sem,
    mg_sem,
    fz_sem,
    fy_sem,
    fc_sem,
    pg_sem,
    ry3_sem,
    rz3_sem,
):
    g = lax.axis_index("grp")
    s = lax.axis_index("seq")
    nz = n_seq // 4
    nq = n_seq // 2
    z = s // 4
    y = (s // 2) % 2
    c = s % 2
    q = z * 2 + y
    rows = n_seq * SLOT
    half = rows // 2
    tok, feat = llm.shape
    kc = 2 * wout.shape[0]
    hid = wout.shape[1]
    cw = win.shape[1]
    cc = 2 * cw
    vit = vout.shape[1]
    pslot = vout.shape[0]
    phalf = pslot // 2
    fw = fc2.shape[0]
    n_img = owner.shape[1]
    qg = feat // kc
    nt = 256
    fhalf = vit // 2

    def dev(gg, zz, yy, c2):
        return (gg, (zz * 2 + yy) * 2 + c2)

    x_peer = dev(1 - g, z, y, c)
    y_peer = dev(g, z, 1 - y, c)
    c_peer = dev(g, z, y, 1 - c)

    sends = []

    def remote(src, dst, rsem, device):
        cp = pltpu.make_async_remote_copy(
            src_ref=src,
            dst_ref=dst,
            send_sem=send_sem.at[len(sends)],
            recv_sem=rsem,
            device_id=device,
            device_id_type=MESH,
        )
        sends.append(cp)
        return cp

    def arrive(dst, rsem):
        pltpu.make_async_copy(dst, dst, rsem).wait()

    barrier = pltpu.get_barrier_semaphore()

    @pl.loop(0, n_grp * n_seq)
    def _(i):
        @pl.when(i != g * n_seq + s)
        def _():
            pl.semaphore_signal(
                barrier, inc=1, device_id=(i // n_seq, i % n_seq), device_id_type=MESH
            )

    loads = {}

    def load(name, src, dst):
        cp = pltpu.make_async_copy(src, dst, ld_sem.at[len(loads)])
        cp.start()
        loads[name] = cp

    for i in range(qg):
        load(("llm", i), llm.at[:, pl.ds(i * kc, kc)], llm_v.at[:, pl.ds(i * kc, kc)])
    load("vpre", vpre, vpre_v)
    load("mpre", mpre, mpre_v)
    wo_own = wo.at[pl.ds(pl.multiple_of(c * (kc // 2), 16), kc // 2)]
    load("wo", wout, wo_own)
    load("wi", win, wi2.at[c])
    load("wf", fc2, wf.at[s])
    load("vout", vout.at[pl.ds(pl.multiple_of(g * phalf, 16), phalf)], vout_v)

    r = iota((rows, 1), 0)
    par = small_div(r, half)
    rem = r - par * half
    o2 = small_div(rem, SLOT)
    slot = rem - o2 * SLOT
    img = iota((1, n_img), 1)
    shard_of = small_div(img, n_seq)
    count = (grid[0:1, :] * grid[1:2, :]).astype(F32)
    width = grid[1:2, :].astype(F32)
    starts = start[...].astype(F32)
    owners = owner[...]
    mine = (owners == o2 * 2 + par) & (shard_of == s)
    first = sum_where(mine, jnp.broadcast_to(starts, mine.shape))
    many = sum_where(mine, jnp.broadcast_to(count, mine.shape))
    onehot = ((iota((rows, tok), 1) == first + slot) & (slot < many)).astype(BF16)

    for i in range(qg):
        loads[("llm", i)].wait()
        picked = jnp.dot(
            onehot, llm_v[:, i * kc : (i + 1) * kc], preferred_element_type=F32
        ).astype(BF16)
        rows_all[g * qg + i, 0] = picked[:half]
        rows_all[g * qg + i, 1] = picked[half:]

    pl.semaphore_wait(barrier, n_grp * n_seq - 1)

    xag = []
    for i in range(qg):
        blk = g * qg + i
        cp = remote(rows_all.at[blk], rows_all.at[blk], xag_sem.at[i], x_peer)
        cp.start()
        xag.append(cp)

    def is_self(qq, p):
        return (qq == q) & (p == c)

    selfs = []

    def send_rows(qq, p):
        src = rows_all.at[qq, p]
        cp = remote(src, xin.at[s], xin_sem.at[s], (g, qq * 2 + p))
        me = is_self(qq, p)
        local = pltpu.make_async_copy(src, xin.at[s], xin_sem.at[s])

        @pl.when(jnp.logical_not(me))
        def _():
            cp.start()

        @pl.when(me)
        def _():
            local.start()

        sends.pop()
        sends.append((cp, me))

    for i in range(qg):
        for p in range(2):
            send_rows(g * qg + i, p)

    remote(wout, wo_own, xw_sem.at[0], c_peer).start()
    remote(win, wi2.at[c], xw_sem.at[1], c_peer).start()

    for i in range(qg):
        arrive(rows_all.at[(1 - g) * qg + i], xag_sem.at[i])
        for p in range(2):
            send_rows((1 - g) * qg + i, p)

    loads["vpre"].wait()
    tile = 64 if pslot % 64 == 0 else 16

    @pl.loop(0, pslot // tile)
    def _(i):
        sl = pl.ds(pl.multiple_of(i * tile, tile), tile)
        v = vpre_v[sl, :].astype(F32)
        sq = jax.nn.sigmoid(1.702 * v)
        act[c, sl, :] = (v * sq).astype(BF16)
        fslope[sl, :] = sq + 1.702 * v * sq * (1.0 - sq)

    remote(act.at[c], act.at[c], xw_sem.at[2], c_peer).start()
    loads["mpre"].wait()
    gslope[...] = gelu_slope(mpre_v[...].astype(F32))

    r = iota((half * n_seq, 1), 0)
    oo = small_div(r, rows)
    rem = r - oo * rows
    src_s = small_div(rem, SLOT)
    slot = rem - src_s * SLOT
    yo = small_div(oo, nz)
    zo = oo - yo * nz
    want = src_s * half + (zo * 2 + yo) * SLOT + slot
    perm = (iota((half * n_seq, half * n_seq), 1) == want).astype(BF16)

    loads["wi"].wait()
    arrive(wi2.at[1 - c], xw_sem.at[1])
    wi[...] = jnp.concatenate([wi2[0], wi2[1]], axis=1)
    loads["wo"].wait()
    arrive(wo.at[pl.ds(pl.multiple_of((1 - c) * (kc // 2), 16), kc // 2)], xw_sem.at[0])

    for src in range(n_seq):
        arrive(xin.at[src], xin_sem.at[src])
        xflat[src * half : (src + 1) * half, :] = xin[src].astype(F32)

    @pl.loop(0, kc // nt)
    def _(t):
        sl = pl.ds(pl.multiple_of(t * nt, nt), nt)
        xperm[:, sl] = jnp.dot(
            perm, xflat[:, sl].astype(BF16), preferred_element_type=F32
        ).astype(BF16)

    hrows = nz * rows

    def part1(yy, out):
        lhs = xperm[pl.ds(pl.multiple_of(yy * hrows, 16), hrows), :]

        @pl.loop(0, hid // nt)
        def _(t):
            sl = pl.ds(pl.multiple_of(t * nt, nt), nt)
            got = jnp.dot(lhs, wo[:, sl], preferred_element_type=F32)
            for zz in range(nz):
                out[zz, :, sl] = got[zz * rows : (zz + 1) * rows].astype(out.dtype)

    part1(1 - y, ys)
    order = [d for d in range(1, nz)] + [0]
    for d in order:
        zz = (z + d) % nz
        remote(ys.at[zz], ry.at[zz], ry_sem.at[d], y_peer).start()
    part1(y, own1)
    for d in order:
        zz = (z + d) % nz
        arrive(ry.at[zz], ry_sem.at[d])
        total = own1[zz] + ry[zz].astype(F32)
        if d:
            zs[d] = total.astype(BF16)
            remote(zs.at[d], rz.at[d], rz_sem.at[d], dev(g, zz, y, c)).start()
        else:
            unit = total
    for d in range(1, nz):
        arrive(rz.at[d], rz_sem.at[d])
        unit = unit + rz[d].astype(F32)
    pre = (gslope[...] * unit.astype(BF16).astype(F32)).astype(BF16)
    allp[q] = pre

    remote(allp.at[q], allp.at[q], agy_sem.at[0], y_peer).start()
    for d in range(1, nz):
        remote(allp.at[q], allp.at[q], agz_sem.at[d], dev(g, (z + d) % nz, y, c)).start()
    for d in range(1, nz):
        qq = ((z + nz - d) % nz) * 2 + y
        arrive(allp.at[qq], agz_sem.at[d])
        remote(allp.at[qq], allp.at[qq], agy_sem.at[d], y_peer).start()

    for d in range(nz):
        zz = (z + nz - d) % nz
        arrive(allp.at[zz * 2 + 1 - y], agy_sem.at[d])
        for yo in range(2):
            p2[yo * rows : (yo + 1) * rows, :] = jnp.dot(
                allp[zz * 2 + yo], wi[...], preferred_element_type=F32
            )
        for e in range(2):
            yo = y + e - 2 * y * e
            far = pl.ds(pl.multiple_of(yo * rows + (1 - g) * half, 8), half)
            near = pl.ds(pl.multiple_of(yo * rows + g * half, 8), half)
            xs[d, e] = p2[far, :].astype(BF16)
            own2[d, e] = p2[near, :].astype(BF16)
        remote(xs.at[d], rx.at[d], rx_sem.at[d], x_peer).start()

    loads["wf"].wait()
    for d in range(1, nz):
        remote(wf.at[s], wf.at[s], fz_sem.at[d], dev(g, (z + d) % nz, y, c)).start()
    remote(wf.at[s], wf.at[s], fy_sem.at[0], y_peer).start()
    remote(wf.at[s], wf.at[s], fc_sem.at[0, 0], c_peer).start()

    for d in range(nz):
        zz = (z + nz - d) % nz
        arrive(rx.at[d], rx_sem.at[d])
        for e in range(2):
            yo = y + e - 2 * y * e
            total = (own2[d, e].astype(F32) + rx[d, e].astype(F32)).astype(BF16)
            if d == 0 and e == 0:
                mg[q] = total
            else:
                a2s[d, e] = total
                remote(a2s.at[d, e], mg.at[q], mg_sem.at[q], dev(g, zz, yo, c)).start()

    for d in range(1, nz):
        blk = wf.at[dev(g, (z + nz - d) % nz, y, c)[1]]
        arrive(blk, fz_sem.at[d])
        remote(blk, blk, fy_sem.at[d], y_peer).start()
        remote(blk, blk, fc_sem.at[0, d], c_peer).start()

    shape = (phalf, phalf)
    r = iota((phalf, 1), 0)
    src_r = small_div(r, 4 * SLOT)
    place = r - src_r * (4 * SLOT)
    mine = (owners == s) & (shard_of == src_r + g * (n_seq // 2))
    many = sum_where(mine, jnp.broadcast_to(count, mine.shape))
    wide = sum_where(mine, jnp.broadcast_to(width, mine.shape))
    col = iota(shape, 1)
    comp = small_div(col, half)
    rem = col - comp * half
    src_c = small_div(rem, SLOT)
    slot = rem - src_c * SLOT
    row_in = jnp.zeros(shape, jnp.int32)
    for k in range(1, SLOT):
        row_in = row_in + (slot >= k * wide).astype(jnp.int32)
    col_in = slot - row_in * wide
    upper = comp >> 1
    target = (2 * row_in + upper) * (2 * wide) + 2 * col_in + (comp - 2 * upper)
    table = ((src_c == src_r) & (slot < many) & (target == place)).astype(BF16)
    loads["vout"].wait()

    per = vit // cc
    for qq in range(nq):

        @pl.when(qq != q)
        def _():
            arrive(mg.at[qq], mg_sem.at[qq])

        part, piece = qq // per, qq % per
        m4[part * half : (part + 1) * half, piece * cc : (piece + 1) * cc] = mg[qq].astype(F32)
    patch_in = jnp.dot(table, m4[...].astype(BF16), preferred_element_type=F32)
    pg = norm_backward(patch_in, vout_v[...].astype(F32), gain[...]).astype(BF16)
    own_rows = pgall.at[c, g]
    pgall[c, g] = pg
    remote(own_rows, own_rows, pg_sem.at[0], x_peer).start()
    remote(own_rows, own_rows, pg_sem.at[1], c_peer).start()
    put_pg = pltpu.make_async_copy(own_rows, pg_out, out_sem.at[0])
    put_pg.start()

    for d in range(nz):
        blk = wf.at[dev(g, (z + nz - d) % nz, 1 - y, c)[1]]
        arrive(blk, fy_sem.at[d])
        remote(blk, blk, fc_sem.at[1, d], c_peer).start()

    far_rows = pgall.at[c, 1 - g]
    arrive(far_rows, pg_sem.at[0])
    remote(far_rows, far_rows, pg_sem.at[2], c_peer).start()
    arrive(act.at[1 - c], xw_sem.at[2])
    arrive(pgall.at[1 - c, g], pg_sem.at[1])
    arrive(pgall.at[1 - c, 1 - g], pg_sem.at[2])

    lane = pl.multiple_of(c * fhalf, 128)
    quarter = 2 * fw
    zh = nz // 2
    lhs = [
        pgall[i, j, :, pl.ds(lane, fhalf)].T for i in range(2) for j in range(2)
    ]
    lhs = jnp.concatenate(lhs, axis=1)
    own3[...] = jnp.dot(
        lhs, jnp.concatenate([act[0], act[1]], axis=0), preferred_element_type=F32
    )
    for zz in range(zh):
        base = pl.multiple_of((zz * 2 + 1 - y) * quarter, 16)
        for c2 in range(2):
            y3s[zz, c2] = own3[pl.ds(base + c2 * fw, fw), :].astype(BF16)
            remote(y3s.at[zz, c2], ry3.at[zz, c2], ry3_sem.at[zz, c2], y_peer).start()
    for zz in range(zh):
        base = pl.multiple_of((zz * 2 + y) * quarter, 16)
        for c2 in range(2):
            arrive(ry3.at[zz, c2], ry3_sem.at[zz, c2])
            total = own3[pl.ds(base + c2 * fw, fw), :] + ry3[zz, c2].astype(F32)
            to_z = c * zh + zz
            me = (to_z == z) & (c2 == c)
            z3s[zz, c2] = total.astype(BF16)
            cp = remote(z3s.at[zz, c2], rz3.at[z], rz3_sem.at[z], dev(g, to_z, y, c2))

            @pl.when(me)
            def _():
                rz3[z] = total.astype(BF16)

            @pl.when(jnp.logical_not(me))
            def _():
                cp.start()

            sends.pop()
            sends.append((cp, me))

    for d in range(nz):
        for e in range(2):
            yy = y + e - 2 * y * e
            arrive(wf.at[dev(g, (z + nz - d) % nz, yy, 1 - c)[1]], fc_sem.at[e, d])
    own_pg = jnp.concatenate([pgall[c, 0], pgall[c, 1]], axis=0)
    wfull = wf.reshape(vit, hid)

    @pl.loop(0, hid // nt)
    def _(t):
        sl = pl.ds(pl.multiple_of(t * nt, nt), nt)
        got = jnp.dot(own_pg, wfull[:, sl], preferred_element_type=F32)
        fc1_v[:, sl] = (fslope[:, sl] * got).astype(BF16)

    put_fc1 = pltpu.make_async_copy(fc1_v, fc1_out, out_sem.at[1])
    put_fc1.start()

    total = jnp.zeros((fw, hid), F32)
    for zz in range(nz):

        @pl.when(jnp.logical_not((zz == z) & (c == z // zh)))
        def _():
            arrive(rz3.at[zz], rz3_sem.at[zz])

        total = total + rz3[zz].astype(F32)
    wg_v[...] = total
    put_wg = pltpu.make_async_copy(wg_v, wg_out, out_sem.at[2])
    put_wg.start()

    for item in sends:
        if isinstance(item, tuple):
            cp, me = item

            @pl.when(jnp.logical_not(me))
            def _():
                cp.wait_send()

        else:
            item.wait_send()
    put_pg.wait()
    put_fc1.wait()
    put_wg.wait()


def fused_on_device(
    llm_grad,
    image_grid,
    image_owner,
    row_start,
    merger_pre,
    vit_out,
    vit_pre,
    ln_gain,
    merger_out_w,
    merger_in_w,
    vit_fc2_w,
    *,
    n_grp,
    n_seq,
):
    n_img = image_owner.shape[0]
    tok, feat = llm_grad.shape
    kb, hid = merger_out_w.shape
    cw = merger_in_w.shape[1]
    pslot, _, vit = vit_out.shape
    fw = vit_fc2_w.shape[0]
    rows = merger_pre.shape[0]
    half, phalf = rows // 2, pslot // 2
    nz, nq, kc, cc = n_seq // 4, n_seq // 2, 2 * kb, 2 * cw
    qg = feat // kc
    vmem, anyspace = pltpu.VMEM, pl.BlockSpec(memory_space=pl.ANY)
    vspec = pl.BlockSpec(memory_space=pltpu.VMEM)
    dma = pltpu.SemaphoreType.DMA
    scratch = [
        vmem((tok, feat), BF16),
        vmem((rows, hid), BF16),
        vmem((phalf, vit), BF16),
        vmem((pslot, hid), BF16),
        vmem((kc, hid), BF16),
        vmem((2, hid, cw), BF16),
        vmem((hid, cc), BF16),
        vmem((n_seq, fw, hid), BF16),
        vmem((2, pslot, hid), BF16),
        vmem((pslot, hid), F32),
        vmem((rows, hid), F32),
        vmem((nq, 2, half, kc), BF16),
        vmem((n_seq, half, kc), BF16),
        vmem((n_seq * half, kc), F32),
        vmem((n_seq * half, kc), BF16),
        vmem((nz, rows, hid), BF16),
        vmem((nz, rows, hid), F32),
        vmem((nz, rows, hid), BF16),
        vmem((nz, rows, hid), BF16),
        vmem((nz, rows, hid), BF16),
        vmem((nq, rows, hid), BF16),
        vmem((2 * rows, cc), F32),
        vmem((nz, 2, half, cc), BF16),
        vmem((nz, 2, half, cc), BF16),
        vmem((nz, 2, half, cc), BF16),
        vmem((nz, 2, half, cc), BF16),
        vmem((nq, half, cc), BF16),
        vmem((phalf, vit), F32),
        vmem((2, 2, phalf, vit), BF16),
        vmem((pslot, hid), BF16),
        vmem((vit // 2, hid), F32),
        vmem((nz // 2, 2, fw, hid), BF16),
        vmem((nz // 2, 2, fw, hid), BF16),
        vmem((nz // 2, 2, fw, hid), BF16),
        vmem((nz, fw, hid), BF16),
        vmem((fw, hid), F32),
        dma((qg + 6,)),
        dma((3,)),
        dma((256,)),
        dma((3,)),
        dma((qg,)),
        dma((n_seq,)),
        dma((nz,)),
        dma((nz,)),
        dma((nz,)),
        dma((nz,)),
        dma((nz,)),
        dma((nq,)),
        dma((nz,)),
        dma((nz,)),
        dma((2, nz)),
        dma((3,)),
        dma((nz // 2, 2)),
        dma((nz,)),
    ]
    pg, fc1, wg = pl.pallas_call(
        functools.partial(fused_kernel, n_grp, n_seq),
        out_shape=(
            jax.ShapeDtypeStruct((phalf, vit), BF16),
            jax.ShapeDtypeStruct((pslot, hid), BF16),
            jax.ShapeDtypeStruct((fw, hid), F32),
        ),
        in_specs=[
            anyspace,
            vspec,
            vspec,
            vspec,
            anyspace,
            anyspace,
            anyspace,
            vspec,
            anyspace,
            anyspace,
            anyspace,
        ],
        out_specs=(anyspace, anyspace, anyspace),
        scratch_shapes=scratch,
        compiler_params=pltpu.CompilerParams(
            collective_id=0, has_side_effects=True, vmem_limit_bytes=60 * 1024 * 1024
        ),
    )(
        llm_grad,
        image_grid.T,
        image_owner.reshape(1, n_img),
        row_start.reshape(1, n_img),
        merger_pre.reshape(rows, hid),
        vit_out.reshape(pslot, vit),
        vit_pre.reshape(pslot, hid),
        ln_gain.reshape(1, vit),
        merger_out_w,
        merger_in_w,
        vit_fc2_w,
    )
    return pg.reshape(phalf, 1, vit), fc1.reshape(pslot, 1, hid), wg


def solution(mesh):
    n_grp, n_seq = mesh.shape["grp"], mesh.shape["seq"]

    def step(*args):
        llm_grad, merger_pre, vit_out = args[0], args[4], args[5]
        merger_out_w, merger_in_w, vit_fc2_w = args[8], args[9], args[10]
        feat, (kb, hid), cw = llm_grad.shape[1], merger_out_w.shape, merger_in_w.shape[1]
        vit, fw, rows = vit_out.shape[2], vit_fc2_w.shape[0], merger_pre.shape[0]
        fits = (
            n_grp == 2
            and n_seq % 8 == 0
            and feat % (2 * kb) == 0
            and kb % 128 == 0
            and hid % 256 == 0
            and (2 * cw) % 128 == 0
            and vit % (2 * cw) == 0
            and vit % 256 == 0
            and fw % 16 == 0
            and rows == n_seq * SLOT
            and rows % 16 == 0
        )
        if fits:
            return fused_on_device(*args, n_grp=n_grp, n_seq=n_seq)
        return on_device(*args)

    return jax.shard_map(
        step,
        mesh=mesh,
        in_specs=(
            P("seq", "grp"),
            P(),
            P(),
            P(),
            P(None, "seq", "grp"),
            P(None, "seq", None),
            P(None, "seq", "grp"),
            P(),
            P("seq", "grp"),
            P("grp", "seq"),
            P("seq", "grp"),
        ),
        out_specs=(P("grp", "seq", None), P(None, "seq", "grp"), P("seq", "grp")),
        check_vma=False,
    )
```

```python
import functools

import jax
import jax.numpy as jnp
from jax import lax
from jax.experimental import pallas as pl
from jax.experimental.pallas import tpu as pltpu
from jax.sharding import PartitionSpec as P

SLOT = 3
MESH = pl.DeviceIdType.MESH
F32 = jnp.float32
BF16 = jnp.bfloat16


def gelu_slope(values):
    return (
        0.5 * (1.0 + lax.erf(values * 0.7071067811865476))
        + values * jnp.exp(-0.5 * values * values) * 0.3989422804014327
    )


def patch_table(widths, counts, slots):
    places = jnp.arange(4 * slots, dtype=jnp.int32)
    merged = places // 4
    corner = places % 4
    row_in = merged[None, :] // widths[:, None]
    col_in = merged[None, :] % widths[:, None]
    target = (
        (2 * row_in + corner[None, :] // 2) * (2 * widths[:, None])
        + 2 * col_in
        + corner[None, :] % 2
    )
    usable = merged[None, :] < counts[:, None]
    return ((target[:, None, :] == places[None, :, None]) & usable[:, None, :]).astype(jnp.float32)


def norm_backward(upstream, inputs, scales):
    average = jnp.mean(inputs, -1, keepdims=True)
    centred = inputs - average
    inverse_std = lax.rsqrt(jnp.mean(centred * centred, -1, keepdims=True) + 1e-06)
    normed = centred * inverse_std
    scaled = upstream * scales
    return inverse_std * (
        scaled
        - jnp.mean(scaled, -1, keepdims=True)
        - normed * jnp.mean(scaled * normed, -1, keepdims=True)
    )


def on_device(
    llm_grad,
    image_grid,
    image_owner,
    row_start,
    merger_pre,
    vit_out,
    vit_pre,
    ln_gain,
    merger_out_w,
    merger_in_w,
    vit_fc2_w,
):
    seq_count = lax.axis_size("seq")
    own_index = lax.axis_index("seq")
    grids = image_grid.reshape(seq_count, seq_count, 2)
    counts = grids[:, :, 0] * grids[:, :, 1]
    widths = grids[:, :, 1]
    owners = image_owner.reshape(seq_count, seq_count)
    starts = row_start.reshape(seq_count, seq_count)
    within = jnp.arange(SLOT, dtype=jnp.int32)
    peers = jnp.arange(seq_count, dtype=jnp.int32)
    shard_rows = llm_grad.shape[0]
    my_owners = lax.dynamic_index_in_dim(owners, own_index, 0, keepdims=False)
    my_counts = lax.dynamic_index_in_dim(counts, own_index, 0, keepdims=False)
    my_starts = lax.dynamic_index_in_dim(starts, own_index, 0, keepdims=False)
    targets = (my_owners[None, :] == peers[:, None]).astype(jnp.int32)
    send_counts = jnp.sum(targets * my_counts[None, :], 1)
    send_starts = jnp.sum(targets * my_starts[None, :], 1)
    indices = jnp.minimum(send_starts[:, None] + within[None, :], shard_rows - 1)
    usable = within[None, :] < send_counts[:, None]
    picked = jnp.take(llm_grad, indices.reshape(-1), axis=0)
    outgoing = jnp.where(usable.reshape(-1, 1), picked, jnp.zeros_like(picked)).reshape(
        seq_count, SLOT, llm_grad.shape[1]
    )
    received = (owners == own_index).astype(jnp.int32)
    recv_counts = jnp.sum(received * counts, 1)
    recv_widths = jnp.sum(received * widths, 1)
    wide_rows = lax.all_gather(
        outgoing.reshape(-1, llm_grad.shape[1]), "grp", axis=1, tiled=True
    )
    sliced = lax.all_to_all(wide_rows, "seq", split_axis=1, concat_axis=0, tiled=True)
    features = sliced.shape[1]
    by_owner = jnp.swapaxes(
        sliced.reshape(seq_count, seq_count, SLOT, features), 0, 1
    ).reshape(-1, features)
    folded = jnp.dot(by_owner, merger_out_w, preferred_element_type=jnp.float32)
    arrived = lax.all_to_all(
        folded.astype(jnp.bfloat16), "seq", split_axis=0, concat_axis=0, tiled=True
    )
    unit_grad = jnp.sum(
        arrived.reshape(seq_count, seq_count * SLOT, -1).astype(jnp.float32), 0
    ).astype(jnp.bfloat16)
    pre_act = merger_pre[:, 0, :].astype(jnp.float32)
    pre_grad = (gelu_slope(pre_act) * unit_grad.astype(jnp.float32)).astype(jnp.bfloat16)
    all_pre = lax.all_gather(pre_grad, "seq", axis=0, tiled=True)
    part_cols = jnp.dot(all_pre, merger_in_w, preferred_element_type=jnp.float32)
    part_rows = lax.all_to_all(
        part_cols.astype(jnp.bfloat16), "seq", split_axis=0, concat_axis=1, tiled=True
    )
    merged_part = jnp.sum(
        lax.all_gather(part_rows, "grp", axis=0).astype(jnp.float32), 0
    )
    vit_width = vit_out.shape[2]
    table = patch_table(recv_widths, recv_counts, SLOT)
    patch_in = jnp.einsum(
        "spq,sqc->spc",
        table,
        merged_part.reshape(seq_count, 4 * SLOT, vit_width),
        precision=lax.Precision.HIGHEST,
    ).reshape(-1, vit_width)
    patch_grad = norm_backward(patch_in, vit_out[:, 0, :].astype(jnp.float32), ln_gain).astype(
        jnp.bfloat16
    )
    group_rows = patch_grad.shape[0] // lax.axis_size("grp")
    own_rows = lax.dynamic_slice_in_dim(
        patch_grad, lax.axis_index("grp") * group_rows, group_rows, 0
    )
    act_grad = jnp.dot(
        patch_grad,
        lax.all_gather(vit_fc2_w, "seq", axis=0, tiled=True),
        preferred_element_type=jnp.float32,
    )
    fc_in = vit_pre[:, 0, :].astype(jnp.float32)
    sigmoid_q = jax.nn.sigmoid(1.702 * fc_in)
    activation = (fc_in * sigmoid_q).astype(jnp.bfloat16)
    fc1_grad = ((sigmoid_q + 1.702 * fc_in * sigmoid_q * (1.0 - sigmoid_q)) * act_grad).astype(
        jnp.bfloat16
    )
    weight_part = lax.dot_general(
        patch_grad, activation, (((0,), (0,)), ((), ())), preferred_element_type=jnp.float32
    )
    weight_parts = lax.all_to_all(
        weight_part.astype(jnp.bfloat16), "seq", split_axis=0, concat_axis=0, tiled=True
    )
    weight_grad = jnp.sum(
        weight_parts.reshape(seq_count, -1, weight_part.shape[1]).astype(jnp.float32), 0
    )
    return (
        own_rows.reshape(group_rows, 1, vit_width),
        fc1_grad.reshape(-1, 1, vit_pre.shape[2]),
        weight_grad,
    )


def small_div(values, by):
    return (values * ((65536 + by - 1) // by)) >> 16


def iota(shape, dim):
    return lax.broadcasted_iota(jnp.int32, shape, dim)


def sum_where(mask, values):
    return jnp.sum(jnp.where(mask, values, 0.0), 1, keepdims=True).astype(jnp.int32)


def fused_kernel(
    n_grp,
    n_seq,
    llm,
    grid,
    owner,
    start,
    mpre,
    vout,
    vpre,
    gain,
    wout,
    win,
    fc2,
    pg_out,
    fc1_out,
    wg_out,
    grid_v,
    owner_v,
    start_v,
    gain_v,
    llm_v,
    mpre_v,
    vout_v,
    vpre_v,
    wo,
    wi,
    wf,
    act,
    fslope,
    gslope,
    rows_all,
    relay,
    xin,
    xflat,
    xperm,
    ys,
    own1,
    ry,
    zs,
    rz,
    allp,
    p2,
    xs,
    own2,
    rx,
    a2s,
    mg,
    m4,
    pgall,
    own3,
    y3s,
    ry3,
    z3s,
    rz3,
    ld_sem,
    send_sem,
    xw_sem,
    xag_sem,
    xin_sem,
    ry_sem,
    rz_sem,
    agz_sem,
    agy_sem,
    rx_sem,
    mg_sem,
    fz_sem,
    fy_sem,
    fc_sem,
    pgx_sem,
    pgc_sem,
    ry3_sem,
    rz3_sem,
):
    g = lax.axis_index("grp")
    s = lax.axis_index("seq")
    nz = n_seq // 4
    nq = n_seq // 2
    z = s // 4
    y = (s // 2) % 2
    c = s % 2
    q = z * 2 + y
    rows = n_seq * SLOT
    half = rows // 2
    tok, feat = llm.shape
    kc = 2 * wout.shape[0]
    hid = wout.shape[1]
    cw = win.shape[0]
    cc = 2 * cw
    vit = vout.shape[1]
    pslot = vout.shape[0]
    phalf = pslot // 2
    fw = fc2.shape[0]
    n_img = owner.shape[1]
    qg = feat // kc
    nt = 256
    fhalf = vit // 2
    first_lanes = -(-fhalf // 256) * 128

    def dev(gg, zz, yy, c2):
        return (gg, (zz * 2 + yy) * 2 + c2)

    x_peer = dev(1 - g, z, y, c)
    y_peer = dev(g, z, 1 - y, c)
    c_peer = dev(g, z, y, 1 - c)

    def zrel(d):
        out = z
        for k in range(nz.bit_length() - 1):
            if d >> k & 1:
                out = out + (1 << k) * (1 - 2 * (z // (1 << k) % 2))
        return out

    sends = []

    def remote(src, dst, rsem, device):
        cp = pltpu.make_async_remote_copy(
            src_ref=src,
            dst_ref=dst,
            send_sem=send_sem.at[len(sends)],
            recv_sem=rsem,
            device_id=device,
            device_id_type=MESH,
        )
        sends.append(cp)
        return cp

    def arrive(dst, rsem):
        pltpu.make_async_copy(dst, dst, rsem).wait()

    def fc2_block(zz, yy, cc2):
        return wf.at[dev(g, zz, yy, cc2)[1]]

    def fc2_z(d):
        own = wf.at[s]
        remote(own, own, fz_sem.at[d], dev(g, zrel(d), y, c)).start()

    def fc2_near():
        own = wf.at[s]
        remote(own, own, fy_sem.at[0], y_peer).start()
        remote(own, own, fc_sem.at[0, 0], c_peer).start()

    def fc2_y(d):
        blk = fc2_block(zrel(d), y, c)
        arrive(blk, fz_sem.at[d])
        remote(blk, blk, fy_sem.at[d], y_peer).start()
        remote(blk, blk, fc_sem.at[0, d], c_peer).start()

    def fc2_core(d):
        blk = fc2_block(zrel(d), 1 - y, c)
        arrive(blk, fy_sem.at[d])
        remote(blk, blk, fc_sem.at[1, d], c_peer).start()

    barrier = pltpu.get_barrier_semaphore()

    @pl.loop(0, n_grp * n_seq)
    def _(i):
        @pl.when(i != g * n_seq + s)
        def _():
            pl.semaphore_signal(
                barrier, inc=1, device_id=(i // n_seq, i % n_seq), device_id_type=MESH
            )

    loads = {}

    def load(name, src, dst):
        cp = pltpu.make_async_copy(src, dst, ld_sem.at[len(loads)])
        cp.start()
        loads[name] = cp

    load("grid", grid, grid_v)
    load("owner", owner, owner_v)
    load("start", start, start_v)
    for i in range(qg):
        load(("llm", i), llm.at[:, pl.ds(i * kc, kc)], llm_v.at[:, pl.ds(i * kc, kc)])
    load("gain", gain, gain_v)
    load("vpre", vpre, vpre_v)
    load("mpre", mpre, mpre_v)
    wo_own = wo.at[pl.ds(pl.multiple_of(c * (kc // 2), 16), kc // 2)]
    load("wo", wout, wo_own)
    wi_own = wi.at[pl.ds(pl.multiple_of(c * cw, 16), cw)]
    wi_far = wi.at[pl.ds(pl.multiple_of((1 - c) * cw, 16), cw)]
    load("wi", win, wi_own)
    load("wf", fc2, wf.at[s])
    load("vout", vout.at[pl.ds(pl.multiple_of(g * phalf, 16), phalf)], vout_v)

    r = iota((rows, 1), 0)
    par = small_div(r, half)
    rem = r - par * half
    o2 = small_div(rem, SLOT)
    slot = rem - o2 * SLOT
    img = iota((1, n_img), 1)
    for name in ("grid", "owner", "start"):
        loads[name].wait()
    shard_of = small_div(img, n_seq)
    count = (grid_v[0:1, :] * grid_v[1:2, :]).astype(F32)
    width = grid_v[1:2, :].astype(F32)
    starts = start_v[...].astype(F32)
    owners = owner_v[...]
    mine = (owners == o2 * 2 + par) & (shard_of == s)
    first = sum_where(mine, jnp.broadcast_to(starts, mine.shape))
    many = sum_where(mine, jnp.broadcast_to(count, mine.shape))
    onehot = ((iota((rows, tok), 1) == first + slot) & (slot < many)).astype(BF16)

    for i in range(qg):
        loads[("llm", i)].wait()
        picked = jnp.dot(
            onehot, llm_v[:, i * kc : (i + 1) * kc], preferred_element_type=F32
        ).astype(BF16)
        rows_all[i, 0] = picked[:half]
        rows_all[i, 1] = picked[half:]

    pl.semaphore_wait(barrier, n_grp * n_seq - 1)

    for i in range(qg):
        remote(rows_all.at[i, 1], relay.at[i], xag_sem.at[i], x_peer).start()

    def unless(me, cp):
        @pl.when(jnp.logical_not(me))
        def _():
            cp.start()

        sends.pop()
        sends.append((cp, me))

    def send_rows(src, qq, p):
        cp = remote(src, xin.at[s], xin_sem.at[s], (g, qq * 2 + p))
        me = (qq == q) & (p == c)

        @pl.when(me)
        def _():
            pltpu.make_async_copy(src, xin.at[s], xin_sem.at[s]).start()

        unless(me, cp)

    for i in range(qg):
        send_rows(rows_all.at[i, 0], g * qg + i, 0)

    loads["wf"].wait()
    remote(wout, wo_own, xw_sem.at[0], c_peer).start()
    remote(win, wi_own, xw_sem.at[1], c_peer).start()

    for i in range(qg):
        arrive(relay.at[i], xag_sem.at[i])
        send_rows(relay.at[i], (1 - g) * qg + i, 1)

    fc2_z(1)
    fc2_z(3)
    fc2_near()
    loads["vpre"].wait()
    tile = 64 if pslot % 64 == 0 else 16

    @pl.loop(0, pslot // tile)
    def _(i):
        sl = pl.ds(pl.multiple_of(i * tile, tile), tile)
        v = vpre_v[sl, :].astype(F32)
        sq = jax.nn.sigmoid(1.702 * v)
        act[c, sl, :] = (v * sq).astype(BF16)
        fslope[sl, :] = sq + 1.702 * v * sq * (1.0 - sq)

    remote(act.at[c], act.at[c], xw_sem.at[2], c_peer).start()
    loads["mpre"].wait()
    gslope[...] = gelu_slope(mpre_v[...].astype(F32))

    r = iota((half * n_seq, 1), 0)
    oo = small_div(r, rows)
    rem = r - oo * rows
    src_s = small_div(rem, SLOT)
    slot = rem - src_s * SLOT
    yo = small_div(oo, nz)
    zo = oo - yo * nz
    want = src_s * half + (zo * 2 + yo) * SLOT + slot
    perm = (iota((half * n_seq, half * n_seq), 1) == want).astype(BF16)

    loads["wi"].wait()
    arrive(wi_far, xw_sem.at[1])
    loads["wo"].wait()
    arrive(wo.at[pl.ds(pl.multiple_of((1 - c) * (kc // 2), 16), kc // 2)], xw_sem.at[0])

    first_hand = (g + c + q // qg) % 2 == 0
    for d in range(nz):
        for k in range(4):
            src = zrel(d) * 4 + k
            arrive(xin.at[src], xin_sem.at[src])
            unless(
                jnp.logical_not(first_hand),
                remote(xin.at[src], xin.at[src], xin_sem.at[src], x_peer),
            )
            at = pl.ds(pl.multiple_of(src * half, 8), half)
            xflat[at, :] = xin[src].astype(F32)

    @pl.loop(0, kc // nt)
    def _(t):
        sl = pl.ds(pl.multiple_of(t * nt, nt), nt)
        xperm[:, sl] = jnp.dot(
            perm, xflat[:, sl].astype(BF16), preferred_element_type=F32
        ).astype(BF16)

    hrows = nz * rows

    def part1(yy, out):
        lhs = xperm[pl.ds(pl.multiple_of(yy * hrows, 16), hrows), :]

        @pl.loop(0, hid // nt)
        def _(t):
            sl = pl.ds(pl.multiple_of(t * nt, nt), nt)
            got = jnp.dot(lhs, wo[:, sl], preferred_element_type=F32)
            for zz in range(nz):
                out[zz, :, sl] = got[zz * rows : (zz + 1) * rows].astype(out.dtype)

    part1(1 - y, ys)
    order = list(range(nz - 1, -1, -1))
    for d in order:
        zz = zrel(d)
        remote(ys.at[zz], ry.at[zz], ry_sem.at[d], y_peer).start()
    part1(y, own1)
    for d in order:
        zz = zrel(d)
        arrive(ry.at[zz], ry_sem.at[d])
        total = own1[zz] + ry[zz].astype(F32)
        if d:
            zs[d] = total.astype(BF16)
            remote(zs.at[d], rz.at[d], rz_sem.at[d], dev(g, zz, y, c)).start()
        else:
            unit = total
    for d in order[:-1]:
        arrive(rz.at[d], rz_sem.at[d])
        unit = unit + rz[d].astype(F32)
    pre = (gslope[...] * unit.astype(BF16).astype(F32)).astype(BF16)
    allp[q] = pre

    remote(allp.at[q], allp.at[q], agy_sem.at[0], y_peer).start()
    for d in order[:-1]:
        remote(allp.at[q], allp.at[q], agz_sem.at[d], dev(g, zrel(d), y, c)).start()
    near_first = [0] + order[:-1]
    for d in near_first[1:]:
        qq = zrel(d) * 2 + y
        arrive(allp.at[qq], agz_sem.at[d])
        remote(allp.at[qq], allp.at[qq], agy_sem.at[d], y_peer).start()

    fc2_z(2)
    fc2_y(1)
    fc2_y(3)
    for d in near_first:
        zz = zrel(d)
        arrive(allp.at[zz * 2 + 1 - y], agy_sem.at[d])
        for yo in range(2):
            p2[yo * rows : (yo + 1) * rows, :] = lax.dot_general(
                allp[zz * 2 + yo],
                wi[...],
                (((1,), (1,)), ((), ())),
                preferred_element_type=F32,
            )
        for e in range(2):
            yo = y + e - 2 * y * e
            far = pl.ds(pl.multiple_of(yo * rows + (1 - g) * half, 8), half)
            near = pl.ds(pl.multiple_of(yo * rows + g * half, 8), half)
            xs[d, e] = p2[far, :].astype(BF16)
            own2[d, e] = p2[near, :].astype(BF16)
        remote(xs.at[d], rx.at[d], rx_sem.at[d], x_peer).start()

    for d in near_first:
        zz = zrel(d)
        arrive(rx.at[d], rx_sem.at[d])
        for e in range(2):
            yo = y + e - 2 * y * e
            total = (own2[d, e].astype(F32) + rx[d, e].astype(F32)).astype(BF16)
            if d == 0 and e == 0:
                mg[q] = total
            else:
                a2s[d, e] = total
                remote(a2s.at[d, e], mg.at[q], mg_sem.at[q], dev(g, zz, yo, c)).start()

    shape = (phalf, phalf)
    r = iota((phalf, 1), 0)
    src_r = small_div(r, 4 * SLOT)
    place = r - src_r * (4 * SLOT)
    mine = (owners == s) & (shard_of == src_r + g * (n_seq // 2))
    many = sum_where(mine, jnp.broadcast_to(count, mine.shape))
    wide = sum_where(mine, jnp.broadcast_to(width, mine.shape))
    col = iota(shape, 1)
    comp = small_div(col, half)
    rem = col - comp * half
    src_c = small_div(rem, SLOT)
    slot = rem - src_c * SLOT
    row_in = jnp.zeros(shape, jnp.int32)
    for k in range(1, SLOT):
        row_in = row_in + (slot >= k * wide).astype(jnp.int32)
    col_in = slot - row_in * wide
    upper = comp >> 1
    target = (2 * row_in + upper) * (2 * wide) + 2 * col_in + (comp - 2 * upper)
    table = ((src_c == src_r) & (slot < many) & (target == place)).astype(BF16)
    loads["vout"].wait()
    loads["gain"].wait()

    per = vit // cc
    for qq in range(nq):

        @pl.when(qq != q)
        def _():
            arrive(mg.at[qq], mg_sem.at[qq])

        part, piece = qq // per, qq % per
        m4[part * half : (part + 1) * half, piece * cc : (piece + 1) * cc] = mg[qq].astype(F32)
    fc2_y(2)
    scales = jnp.concatenate([gain_v[k : k + 1, :] for k in range(vit // 128)], axis=1)
    patch_in = jnp.dot(table, m4[...].astype(BF16), preferred_element_type=F32)
    pg = norm_backward(patch_in, vout_v[...].astype(F32), scales).astype(BF16)
    pgall[c, g] = pg
    pg_out[...] = pg
    zh = nz // 2
    cuts = [(0, first_lanes), (first_lanes, fhalf - first_lanes)]

    def piece(i, j, side, k):
        lane = pl.multiple_of(side * fhalf + cuts[k][0], 128)
        return pgall.at[i, j, :, pl.ds(lane, cuts[k][1])]

    for k in range(2):
        for side in (1 - c, c):
            at = piece(c, g, side, k)
            is_far = 0 if side is c else 1
            remote(at, at, pgx_sem.at[k, is_far], x_peer).start()
        at = piece(c, g, 1 - c, k)
        remote(at, at, pgc_sem.at[k, 0], c_peer).start()
    fc2_core(0)
    fc2_core(1)
    fc2_core(3)
    arrive(act.at[1 - c], xw_sem.at[2])
    quarter = 2 * fw
    acts = act.reshape(2 * pslot, hid)
    hh = hid // 2
    sent = 0
    for k in range(2):
        at = piece(c, 1 - g, 1 - c, k)
        arrive(at, pgx_sem.at[k, 1])
        remote(at, at, pgc_sem.at[k, 1], c_peer).start()
        arrive(piece(c, 1 - g, c, k), pgx_sem.at[k, 0])
        arrive(piece(1 - c, g, c, k), pgc_sem.at[k, 0])
        arrive(piece(1 - c, 1 - g, c, k), pgc_sem.at[k, 1])
        begin, size = cuts[k]
        lhs = jnp.concatenate(
            [piece(i, j, c, k)[...] for i in range(2) for j in range(2)], axis=0
        )
        ready = zh if k else (begin + size) // (2 * quarter)
        for hf in range(2):
            col = slice(hf * hh, (hf + 1) * hh)
            own3[begin : begin + size, col] = lax.dot_general(
                lhs, acts[:, col], (((0,), (0,)), ((), ())), preferred_element_type=F32
            )
            for zz in range(sent, ready):
                base = pl.multiple_of((zz * 2 + 1 - y) * quarter, 16)
                for c2 in range(2):
                    kk = zz * 2 + c2
                    y3s[hf, kk] = own3[pl.ds(base + c2 * fw, fw), col].astype(BF16)
                    remote(
                        y3s.at[hf, kk], ry3.at[hf, kk], ry3_sem.at[hf, kk], y_peer
                    ).start()
        sent = ready
    for zz in range(zh):
        base = pl.multiple_of((zz * 2 + y) * quarter, 16)
        for hf in range(2):
            col = slice(hf * hh, (hf + 1) * hh)
            for c2 in range(2):
                k = zz * 2 + c2
                arrive(ry3.at[hf, k], ry3_sem.at[hf, k])
                total = own3[pl.ds(base + c2 * fw, fw), col] + ry3[hf, k].astype(F32)
                to_z = c * zh + zz
                me = (to_z == z) & (c2 == c)
                z3s[hf, k] = total.astype(BF16)

                @pl.when(me)
                def _():
                    rz3[z, hf] = total.astype(BF16)

                unless(
                    me,
                    remote(
                        z3s.at[hf, k],
                        rz3.at[z, hf],
                        rz3_sem.at[z, hf],
                        dev(g, to_z, y, c2),
                    ),
                )

    fc2_core(2)
    for d in range(nz):
        for e in range(2):
            yy = y + e - 2 * y * e
            arrive(fc2_block(zrel(d), yy, 1 - c), fc_sem.at[e, d])
    own_pg = jnp.concatenate([pgall[c, 0], pgall[c, 1]], axis=0)
    wfull = wf.reshape(vit, hid)

    @pl.loop(0, hid // nt)
    def _(t):
        sl = pl.ds(pl.multiple_of(t * nt, nt), nt)
        got = jnp.dot(own_pg, wfull[:, sl], preferred_element_type=F32)
        fc1_out[:, sl] = (fslope[:, sl] * got).astype(BF16)

    for hf in range(2):
        total = jnp.zeros((fw, hh), F32)
        for zz in range(nz):

            @pl.when(jnp.logical_not((zz == z) & (c == z // zh)))
            def _():
                arrive(rz3.at[zz, hf], rz3_sem.at[zz, hf])

            total = total + rz3[zz, hf].astype(F32)
        wg_out[:, hf * hh : (hf + 1) * hh] = total

    for item in sends:
        if isinstance(item, tuple):
            cp, me = item

            @pl.when(jnp.logical_not(me))
            def _():
                cp.wait_send()

        else:
            item.wait_send()


def in_hbm(x):
    return pltpu.with_memory_space_constraint(x, pltpu.HBM)


def fused_on_device(
    llm_grad,
    image_grid,
    image_owner,
    row_start,
    merger_pre,
    vit_out,
    vit_pre,
    ln_gain,
    merger_out_w,
    merger_in_w,
    vit_fc2_w,
    *,
    n_grp,
    n_seq,
):
    n_img = image_owner.shape[0]
    tok, feat = llm_grad.shape
    kb, hid = merger_out_w.shape
    cw = merger_in_w.shape[1]
    pslot, _, vit = vit_out.shape
    fw = vit_fc2_w.shape[0]
    rows = merger_pre.shape[0]
    half, phalf = rows // 2, pslot // 2
    nz, nq, kc, cc = n_seq // 4, n_seq // 2, 2 * kb, 2 * cw
    qg = feat // kc
    vmem, anyspace = pltpu.VMEM, pl.BlockSpec(memory_space=pltpu.HBM)
    vspec = pl.BlockSpec(memory_space=pltpu.VMEM)
    dma = pltpu.SemaphoreType.DMA
    scratch = [
        vmem((2, n_img), jnp.int32),
        vmem((1, n_img), jnp.int32),
        vmem((1, n_img), jnp.int32),
        vmem((vit // 128, 128), F32),
        vmem((tok, feat), BF16),
        vmem((rows, hid), BF16),
        vmem((phalf, vit), BF16),
        vmem((pslot, hid), BF16),
        vmem((kc, hid), BF16),
        vmem((cc, hid), BF16),
        vmem((n_seq, fw, hid), BF16),
        vmem((2, pslot, hid), BF16),
        vmem((pslot, hid), F32),
        vmem((rows, hid), F32),
        vmem((qg, 2, half, kc), BF16),
        vmem((qg, half, kc), BF16),
        vmem((n_seq, half, kc), BF16),
        vmem((n_seq * half, kc), F32),
        vmem((n_seq * half, kc), BF16),
        vmem((nz, rows, hid), BF16),
        vmem((nz, rows, hid), F32),
        vmem((nz, rows, hid), BF16),
        vmem((nz, rows, hid), BF16),
        vmem((nz, rows, hid), BF16),
        vmem((nq, rows, hid), BF16),
        vmem((2 * rows, cc), F32),
        vmem((nz, 2, half, cc), BF16),
        vmem((nz, 2, half, cc), BF16),
        vmem((nz, 2, half, cc), BF16),
        vmem((nz, 2, half, cc), BF16),
        vmem((nq, half, cc), BF16),
        vmem((phalf, vit), F32),
        vmem((2, 2, phalf, vit), BF16),
        vmem((vit // 2, hid), F32),
        vmem((2, nz, fw, hid // 2), BF16),
        vmem((2, nz, fw, hid // 2), BF16),
        vmem((2, nz, fw, hid // 2), BF16),
        vmem((nz, 2, fw, hid // 2), BF16),
        dma((qg + 10,)),
        dma((256,)),
        dma((3,)),
        dma((qg,)),
        dma((n_seq,)),
        dma((nz,)),
        dma((nz,)),
        dma((nz,)),
        dma((nz,)),
        dma((nz,)),
        dma((nq,)),
        dma((nz,)),
        dma((nz,)),
        dma((2, nz)),
        dma((2, 2)),
        dma((2, 2)),
        dma((2, nz)),
        dma((nz, 2)),
    ]
    pg, fc1, wg = pl.pallas_call(
        functools.partial(fused_kernel, n_grp, n_seq),
        out_shape=(
            jax.ShapeDtypeStruct((phalf, vit), BF16),
            jax.ShapeDtypeStruct((pslot, hid), BF16),
            jax.ShapeDtypeStruct((fw, hid), F32),
        ),
        in_specs=[anyspace] * 11,
        out_specs=(vspec, vspec, vspec),
        scratch_shapes=scratch,
        compiler_params=pltpu.CompilerParams(
            collective_id=0, has_side_effects=True, vmem_limit_bytes=40 * 1024 * 1024
        ),
    )(
        in_hbm(llm_grad),
        in_hbm(image_grid.T),
        in_hbm(image_owner.reshape(1, n_img)),
        in_hbm(row_start.reshape(1, n_img)),
        in_hbm(merger_pre.reshape(rows, hid)),
        in_hbm(vit_out.reshape(pslot, vit)),
        in_hbm(vit_pre.reshape(pslot, hid)),
        in_hbm(ln_gain.reshape(vit // 128, 128)),
        in_hbm(merger_out_w),
        in_hbm(merger_in_w.T),
        in_hbm(vit_fc2_w),
    )
    return pg.reshape(phalf, 1, vit), fc1.reshape(pslot, 1, hid), wg


def solution(mesh):
    n_grp, n_seq = mesh.shape["grp"], mesh.shape["seq"]

    def step(*args):
        llm_grad, merger_pre, vit_out = args[0], args[4], args[5]
        merger_out_w, merger_in_w, vit_fc2_w = args[8], args[9], args[10]
        feat, (kb, hid), cw = llm_grad.shape[1], merger_out_w.shape, merger_in_w.shape[1]
        vit, fw, rows = vit_out.shape[2], vit_fc2_w.shape[0], merger_pre.shape[0]
        fits = (
            n_grp == 2
            and n_seq >= 8
            and n_seq & (n_seq - 1) == 0
            and feat % (2 * kb) == 0
            and kb % 128 == 0
            and hid % 256 == 0
            and (2 * cw) % 128 == 0
            and vit % (2 * cw) == 0
            and vit % 256 == 0
            and fw % 16 == 0
            and rows == n_seq * SLOT
            and rows % 16 == 0
        )
        if fits:
            return fused_on_device(*args, n_grp=n_grp, n_seq=n_seq)
        return on_device(*args)

    return jax.shard_map(
        step,
        mesh=mesh,
        in_specs=(
            P("seq", "grp"),
            P(),
            P(),
            P(),
            P(None, "seq", "grp"),
            P(None, "seq", None),
            P(None, "seq", "grp"),
            P(),
            P("seq", "grp"),
            P("grp", "seq"),
            P("seq", "grp"),
        ),
        out_specs=(P("grp", "seq", None), P(None, "seq", "grp"), P("seq", "grp")),
        check_vma=False,
    )
```

```python
import functools

import jax
import jax.numpy as jnp
from jax import lax
from jax.experimental import pallas as pl
from jax.experimental.pallas import tpu as pltpu
from jax.sharding import PartitionSpec as P

SLOT = 3
MESH = pl.DeviceIdType.MESH
F32 = jnp.float32
BF16 = jnp.bfloat16


def gelu_slope(values):
    return (
        0.5 * (1.0 + lax.erf(values * 0.7071067811865476))
        + values * jnp.exp(-0.5 * values * values) * 0.3989422804014327
    )


def patch_table(widths, counts, slots):
    places = jnp.arange(4 * slots, dtype=jnp.int32)
    merged = places // 4
    corner = places % 4
    row_in = merged[None, :] // widths[:, None]
    col_in = merged[None, :] % widths[:, None]
    target = (
        (2 * row_in + corner[None, :] // 2) * (2 * widths[:, None])
        + 2 * col_in
        + corner[None, :] % 2
    )
    usable = merged[None, :] < counts[:, None]
    return ((target[:, None, :] == places[None, :, None]) & usable[:, None, :]).astype(jnp.float32)


def norm_backward(upstream, inputs, scales):
    average = jnp.mean(inputs, -1, keepdims=True)
    centred = inputs - average
    inverse_std = lax.rsqrt(jnp.mean(centred * centred, -1, keepdims=True) + 1e-06)
    normed = centred * inverse_std
    scaled = upstream * scales
    return inverse_std * (
        scaled
        - jnp.mean(scaled, -1, keepdims=True)
        - normed * jnp.mean(scaled * normed, -1, keepdims=True)
    )


def on_device(
    llm_grad,
    image_grid,
    image_owner,
    row_start,
    merger_pre,
    vit_out,
    vit_pre,
    ln_gain,
    merger_out_w,
    merger_in_w,
    vit_fc2_w,
):
    seq_count = lax.axis_size("seq")
    own_index = lax.axis_index("seq")
    grids = image_grid.reshape(seq_count, seq_count, 2)
    counts = grids[:, :, 0] * grids[:, :, 1]
    widths = grids[:, :, 1]
    owners = image_owner.reshape(seq_count, seq_count)
    starts = row_start.reshape(seq_count, seq_count)
    within = jnp.arange(SLOT, dtype=jnp.int32)
    peers = jnp.arange(seq_count, dtype=jnp.int32)
    shard_rows = llm_grad.shape[0]
    my_owners = lax.dynamic_index_in_dim(owners, own_index, 0, keepdims=False)
    my_counts = lax.dynamic_index_in_dim(counts, own_index, 0, keepdims=False)
    my_starts = lax.dynamic_index_in_dim(starts, own_index, 0, keepdims=False)
    targets = (my_owners[None, :] == peers[:, None]).astype(jnp.int32)
    send_counts = jnp.sum(targets * my_counts[None, :], 1)
    send_starts = jnp.sum(targets * my_starts[None, :], 1)
    indices = jnp.minimum(send_starts[:, None] + within[None, :], shard_rows - 1)
    usable = within[None, :] < send_counts[:, None]
    picked = jnp.take(llm_grad, indices.reshape(-1), axis=0)
    outgoing = jnp.where(usable.reshape(-1, 1), picked, jnp.zeros_like(picked)).reshape(
        seq_count, SLOT, llm_grad.shape[1]
    )
    received = (owners == own_index).astype(jnp.int32)
    recv_counts = jnp.sum(received * counts, 1)
    recv_widths = jnp.sum(received * widths, 1)
    wide_rows = lax.all_gather(
        outgoing.reshape(-1, llm_grad.shape[1]), "grp", axis=1, tiled=True
    )
    sliced = lax.all_to_all(wide_rows, "seq", split_axis=1, concat_axis=0, tiled=True)
    features = sliced.shape[1]
    by_owner = jnp.swapaxes(
        sliced.reshape(seq_count, seq_count, SLOT, features), 0, 1
    ).reshape(-1, features)
    folded = jnp.dot(by_owner, merger_out_w, preferred_element_type=jnp.float32)
    arrived = lax.all_to_all(
        folded.astype(jnp.bfloat16), "seq", split_axis=0, concat_axis=0, tiled=True
    )
    unit_grad = jnp.sum(
        arrived.reshape(seq_count, seq_count * SLOT, -1).astype(jnp.float32), 0
    ).astype(jnp.bfloat16)
    pre_act = merger_pre[:, 0, :].astype(jnp.float32)
    pre_grad = (gelu_slope(pre_act) * unit_grad.astype(jnp.float32)).astype(jnp.bfloat16)
    all_pre = lax.all_gather(pre_grad, "seq", axis=0, tiled=True)
    part_cols = jnp.dot(all_pre, merger_in_w, preferred_element_type=jnp.float32)
    part_rows = lax.all_to_all(
        part_cols.astype(jnp.bfloat16), "seq", split_axis=0, concat_axis=1, tiled=True
    )
    merged_part = jnp.sum(
        lax.all_gather(part_rows, "grp", axis=0).astype(jnp.float32), 0
    )
    vit_width = vit_out.shape[2]
    table = patch_table(recv_widths, recv_counts, SLOT)
    patch_in = jnp.einsum(
        "spq,sqc->spc",
        table,
        merged_part.reshape(seq_count, 4 * SLOT, vit_width),
        precision=lax.Precision.HIGHEST,
    ).reshape(-1, vit_width)
    patch_grad = norm_backward(patch_in, vit_out[:, 0, :].astype(jnp.float32), ln_gain).astype(
        jnp.bfloat16
    )
    group_rows = patch_grad.shape[0] // lax.axis_size("grp")
    own_rows = lax.dynamic_slice_in_dim(
        patch_grad, lax.axis_index("grp") * group_rows, group_rows, 0
    )
    act_grad = jnp.dot(
        patch_grad,
        lax.all_gather(vit_fc2_w, "seq", axis=0, tiled=True),
        preferred_element_type=jnp.float32,
    )
    fc_in = vit_pre[:, 0, :].astype(jnp.float32)
    sigmoid_q = jax.nn.sigmoid(1.702 * fc_in)
    activation = (fc_in * sigmoid_q).astype(jnp.bfloat16)
    fc1_grad = ((sigmoid_q + 1.702 * fc_in * sigmoid_q * (1.0 - sigmoid_q)) * act_grad).astype(
        jnp.bfloat16
    )
    weight_part = lax.dot_general(
        patch_grad, activation, (((0,), (0,)), ((), ())), preferred_element_type=jnp.float32
    )
    weight_parts = lax.all_to_all(
        weight_part.astype(jnp.bfloat16), "seq", split_axis=0, concat_axis=0, tiled=True
    )
    weight_grad = jnp.sum(
        weight_parts.reshape(seq_count, -1, weight_part.shape[1]).astype(jnp.float32), 0
    )
    return (
        own_rows.reshape(group_rows, 1, vit_width),
        fc1_grad.reshape(-1, 1, vit_pre.shape[2]),
        weight_grad,
    )


def small_div(values, by):
    return (values * ((65536 + by - 1) // by)) >> 16


def iota(shape, dim):
    return lax.broadcasted_iota(jnp.int32, shape, dim)


def sum_where(mask, values):
    return jnp.sum(jnp.where(mask, values, 0.0), 1, keepdims=True).astype(jnp.int32)


def fused_kernel(
    n_grp,
    n_seq,
    llm,
    grid,
    owner,
    start,
    mpre,
    vout,
    vpre,
    gain,
    wout,
    win,
    fc2,
    pg_out,
    fc1_out,
    wg_out,
    grid_v,
    owner_v,
    start_v,
    gain_v,
    llm_v,
    mpre_v,
    vout_v,
    vpre_v,
    wo,
    wi,
    wf,
    act,
    fslope,
    gslope,
    rows_all,
    relay,
    xin,
    xflat,
    xperm,
    ys,
    own1,
    ry,
    zs,
    rz,
    allp,
    p2,
    xs,
    own2,
    rx,
    a2s,
    mg,
    m4,
    pgall,
    own3,
    y3s,
    ry3,
    z3s,
    rz3,
    ld_sem,
    send_sem,
    xw_sem,
    xag_sem,
    xin_sem,
    ry_sem,
    rz_sem,
    agz_sem,
    agy_sem,
    rx_sem,
    mg_sem,
    fz_sem,
    fy_sem,
    fc_sem,
    mgx_sem,
    pgc_sem,
    ry3_sem,
    rz3_sem,
):
    g = lax.axis_index("grp")
    s = lax.axis_index("seq")
    nz = n_seq // 4
    nq = n_seq // 2
    z = s // 4
    y = (s // 2) % 2
    c = s % 2
    q = z * 2 + y
    rows = n_seq * SLOT
    half = rows // 2
    tok, feat = llm.shape
    kc = 2 * wout.shape[0]
    hid = wout.shape[1]
    cw = win.shape[0]
    cc = 2 * cw
    vit = vout.shape[1]
    pslot = vout.shape[0]
    phalf = pslot // 2
    fw = fc2.shape[0]
    n_img = owner.shape[1]
    qg = feat // kc
    nt = 256
    fhalf = vit // 2
    first_lanes = -(-fhalf // 256) * 128

    def dev(gg, zz, yy, c2):
        return (gg, (zz * 2 + yy) * 2 + c2)

    x_peer = dev(1 - g, z, y, c)
    y_peer = dev(g, z, 1 - y, c)
    c_peer = dev(g, z, y, 1 - c)

    def zrel(d):
        out = z
        for k in range(nz.bit_length() - 1):
            if d >> k & 1:
                out = out + (1 << k) * (1 - 2 * (z // (1 << k) % 2))
        return out

    sends = []

    def remote(src, dst, rsem, device):
        cp = pltpu.make_async_remote_copy(
            src_ref=src,
            dst_ref=dst,
            send_sem=send_sem.at[len(sends)],
            recv_sem=rsem,
            device_id=device,
            device_id_type=MESH,
        )
        sends.append(cp)
        return cp

    def arrive(dst, rsem):
        pltpu.make_async_copy(dst, dst, rsem).wait()

    def fc2_block(zz, yy, cc2):
        return wf.at[dev(g, zz, yy, cc2)[1]]

    def fc2_z(d):
        own = wf.at[s]
        remote(own, own, fz_sem.at[d], dev(g, zrel(d), y, c)).start()

    def fc2_near():
        own = wf.at[s]
        remote(own, own, fy_sem.at[0], y_peer).start()
        remote(own, own, fc_sem.at[0, 0], c_peer).start()

    def fc2_y(d):
        blk = fc2_block(zrel(d), y, c)
        arrive(blk, fz_sem.at[d])
        remote(blk, blk, fy_sem.at[d], y_peer).start()
        remote(blk, blk, fc_sem.at[0, d], c_peer).start()

    def fc2_core(d):
        blk = fc2_block(zrel(d), 1 - y, c)
        arrive(blk, fy_sem.at[d])
        remote(blk, blk, fc_sem.at[1, d], c_peer).start()

    barrier = pltpu.get_barrier_semaphore()

    @pl.loop(0, n_grp * n_seq)
    def _(i):
        @pl.when(i != g * n_seq + s)
        def _():
            pl.semaphore_signal(
                barrier, inc=1, device_id=(i // n_seq, i % n_seq), device_id_type=MESH
            )

    loads = {}

    def load(name, src, dst):
        cp = pltpu.make_async_copy(src, dst, ld_sem.at[len(loads)])
        cp.start()
        loads[name] = cp

    load("grid", grid, grid_v)
    load("owner", owner, owner_v)
    load("start", start, start_v)
    for i in range(qg):
        load(("llm", i), llm.at[:, pl.ds(i * kc, kc)], llm_v.at[:, pl.ds(i * kc, kc)])
    load("gain", gain, gain_v)
    load("vpre", vpre, vpre_v)
    load("mpre", mpre, mpre_v)
    wo_own = wo.at[pl.ds(pl.multiple_of(c * (kc // 2), 16), kc // 2)]
    load("wo", wout, wo_own)
    wi_own = wi.at[pl.ds(pl.multiple_of(c * cw, 16), cw)]
    wi_far = wi.at[pl.ds(pl.multiple_of((1 - c) * cw, 16), cw)]
    load("wi", win, wi_own)
    load("wf", fc2, wf.at[s])
    load("vout", vout, vout_v)

    r = iota((rows, 1), 0)
    par = small_div(r, half)
    rem = r - par * half
    o2 = small_div(rem, SLOT)
    slot = rem - o2 * SLOT
    img = iota((1, n_img), 1)
    for name in ("grid", "owner", "start"):
        loads[name].wait()
    shard_of = small_div(img, n_seq)
    count = (grid_v[0:1, :] * grid_v[1:2, :]).astype(F32)
    width = grid_v[1:2, :].astype(F32)
    starts = start_v[...].astype(F32)
    owners = owner_v[...]
    mine = (owners == o2 * 2 + par) & (shard_of == s)
    first = sum_where(mine, jnp.broadcast_to(starts, mine.shape))
    many = sum_where(mine, jnp.broadcast_to(count, mine.shape))
    onehot = ((iota((rows, tok), 1) == first + slot) & (slot < many)).astype(BF16)

    for i in range(qg):
        loads[("llm", i)].wait()
        picked = jnp.dot(
            onehot, llm_v[:, i * kc : (i + 1) * kc], preferred_element_type=F32
        ).astype(BF16)
        rows_all[i, 0] = picked[:half]
        rows_all[i, 1] = picked[half:]

    pl.semaphore_wait(barrier, n_grp * n_seq - 1)

    for i in range(qg):
        remote(rows_all.at[i, 1], relay.at[i], xag_sem.at[i], x_peer).start()

    def unless(me, cp):
        @pl.when(jnp.logical_not(me))
        def _():
            cp.start()

        sends.pop()
        sends.append((cp, me))

    def send_rows(src, qq, p):
        cp = remote(src, xin.at[s], xin_sem.at[s], (g, qq * 2 + p))
        me = (qq == q) & (p == c)

        @pl.when(me)
        def _():
            pltpu.make_async_copy(src, xin.at[s], xin_sem.at[s]).start()

        unless(me, cp)

    for i in range(qg):
        send_rows(rows_all.at[i, 0], g * qg + i, 0)

    loads["wf"].wait()
    remote(wout, wo_own, xw_sem.at[0], c_peer).start()
    remote(win, wi_own, xw_sem.at[1], c_peer).start()

    for i in range(qg):
        arrive(relay.at[i], xag_sem.at[i])
        send_rows(relay.at[i], (1 - g) * qg + i, 1)

    fc2_z(1)
    fc2_z(3)
    fc2_near()
    loads["vpre"].wait()
    tile = 64 if pslot % 64 == 0 else 16

    @pl.loop(0, pslot // tile)
    def _(i):
        sl = pl.ds(pl.multiple_of(i * tile, tile), tile)
        v = vpre_v[sl, :].astype(F32)
        sq = jax.nn.sigmoid(1.702 * v)
        act[c, sl, :] = (v * sq).astype(BF16)
        fslope[sl, :] = sq + 1.702 * v * sq * (1.0 - sq)

    remote(act.at[c], act.at[c], xw_sem.at[2], c_peer).start()
    loads["mpre"].wait()
    gslope[...] = gelu_slope(mpre_v[...].astype(F32))

    r = iota((half * n_seq, 1), 0)
    oo = small_div(r, rows)
    rem = r - oo * rows
    src_s = small_div(rem, SLOT)
    slot = rem - src_s * SLOT
    yo = small_div(oo, nz)
    zo = oo - yo * nz
    want = src_s * half + (zo * 2 + yo) * SLOT + slot
    perm = (iota((half * n_seq, half * n_seq), 1) == want).astype(BF16)

    loads["gain"].wait()
    loads["wi"].wait()
    arrive(wi_far, xw_sem.at[1])
    loads["wo"].wait()
    arrive(wo.at[pl.ds(pl.multiple_of((1 - c) * (kc // 2), 16), kc // 2)], xw_sem.at[0])

    first_hand = (g + c + q // qg) % 2 == 0
    for d in range(nz):
        for k in range(4):
            src = zrel(d) * 4 + k
            arrive(xin.at[src], xin_sem.at[src])
            unless(
                jnp.logical_not(first_hand),
                remote(xin.at[src], xin.at[src], xin_sem.at[src], x_peer),
            )
            at = pl.ds(pl.multiple_of(src * half, 8), half)
            xflat[at, :] = xin[src].astype(F32)

    @pl.loop(0, kc // nt)
    def _(t):
        sl = pl.ds(pl.multiple_of(t * nt, nt), nt)
        xperm[:, sl] = jnp.dot(
            perm, xflat[:, sl].astype(BF16), preferred_element_type=F32
        ).astype(BF16)

    hrows = nz * rows

    hh = hid // 2
    order = list(range(nz - 1, -1, -1))

    def part1(yy, hf, out):
        lhs = xperm[pl.ds(pl.multiple_of(yy * hrows, 16), hrows), :]
        got = jnp.dot(lhs, wo[:, hf * hh : (hf + 1) * hh], preferred_element_type=F32)
        for zz in range(nz):
            out[hf, zz] = got[zz * rows : (zz + 1) * rows].astype(out.dtype)

    for hf in range(2):
        part1(1 - y, hf, ys)
        for d in order:
            zz = zrel(d)
            remote(ys.at[hf, zz], ry.at[hf, zz], ry_sem.at[hf, d], y_peer).start()
    for hf in range(2):
        part1(y, hf, own1)
    units = {}

    def over_y(hf, d):
        zz = zrel(d)
        arrive(ry.at[hf, zz], ry_sem.at[hf, d])
        total = own1[hf, zz] + ry[hf, zz].astype(F32)
        if d:
            zs[hf, d] = total.astype(BF16)
            remote(zs.at[hf, d], rz.at[hf, d], rz_sem.at[hf, d], dev(g, zz, y, c)).start()
        else:
            units[hf] = total

    def over_z(hf):
        unit = units[hf]
        for d in order[:-1]:
            arrive(rz.at[hf, d], rz_sem.at[hf, d])
            unit = unit + rz[hf, d].astype(F32)
        slope = gslope[:, hf * hh : (hf + 1) * hh]
        allp[hf, q] = (slope * unit.astype(BF16).astype(F32)).astype(BF16)
        mine = allp.at[hf, q]
        remote(mine, mine, agy_sem.at[hf, 0], y_peer).start()
        for d in order[:-1]:
            remote(mine, mine, agz_sem.at[hf, d], dev(g, zrel(d), y, c)).start()

    for d in order:
        over_y(0, d)
    for d in order:
        over_y(1, d)
    over_z(0)
    over_z(1)
    fc2_y(1)
    near_first = [0] + order[:-1]
    for hf in range(2):
        for d in near_first[1:]:
            qq = zrel(d) * 2 + y
            arrive(allp.at[hf, qq], agz_sem.at[hf, d])
            remote(allp.at[hf, qq], allp.at[hf, qq], agy_sem.at[hf, d], y_peer).start()

    fc2_z(2)
    fc2_y(3)
    def columns_of(d):
        zz = zrel(d)
        got = jnp.zeros((2 * rows, cc), F32)
        for hf in range(2):
            arrive(allp.at[hf, zz * 2 + 1 - y], agy_sem.at[hf, d])
            got = got + lax.dot_general(
                allp[hf, pl.ds(zz * 2, 2)].reshape(2 * rows, hh),
                wi[:, hf * hh : (hf + 1) * hh],
                (((1,), (1,)), ((), ())),
                preferred_element_type=F32,
            )
        p2[...] = got
        for e in range(2):
            yo = y + e - 2 * y * e
            far = pl.ds(pl.multiple_of(yo * rows + (1 - g) * half, 8), half)
            near = pl.ds(pl.multiple_of(yo * rows + g * half, 8), half)
            xs[d, e] = p2[far, :].astype(BF16)
            own2[d, e] = p2[near, :].astype(BF16)
        remote(xs.at[d], rx.at[d], rx_sem.at[d], x_peer).start()

    def to_owners(d):
        arrive(rx.at[d], rx_sem.at[d])
        for e in (1, 0):
            yo = y + e - 2 * y * e
            total = (own2[d, e].astype(F32) + rx[d, e].astype(F32)).astype(BF16)
            if d == 0 and e == 0:
                mg[g, q] = total
                remote(mg.at[g, q], mg.at[g, q], mgx_sem.at[q], x_peer).start()
            else:
                a2s[d, e] = total
                remote(
                    a2s.at[d, e], mg.at[g, q], mg_sem.at[q], dev(g, zrel(d), yo, c)
                ).start()

    for k, d in enumerate(near_first):
        columns_of(d)
        if k:
            to_owners(near_first[k - 1])
    to_owners(near_first[-1])
    def slot_table(gg):
        shape = (phalf, phalf)
        r = iota((phalf, 1), 0)
        src_r = small_div(r, 4 * SLOT)
        place = r - src_r * (4 * SLOT)
        mine = (owners == s) & (shard_of == src_r + gg * (n_seq // 2))
        many = sum_where(mine, jnp.broadcast_to(count, mine.shape))
        wide = sum_where(mine, jnp.broadcast_to(width, mine.shape))
        col = iota(shape, 1)
        comp = small_div(col, half)
        rem = col - comp * half
        src_c = small_div(rem, SLOT)
        slot = rem - src_c * SLOT
        row_in = jnp.zeros(shape, jnp.int32)
        for k in range(1, SLOT):
            row_in = row_in + (slot >= k * wide).astype(jnp.int32)
        col_in = slot - row_in * wide
        upper = comp >> 1
        target = (2 * row_in + upper) * (2 * wide) + 2 * col_in + (comp - 2 * upper)
        return ((src_c == src_r) & (slot < many) & (target == place)).astype(BF16)

    per = vit // cc
    scales = jnp.concatenate([gain_v[k : k + 1, :] for k in range(vit // 128)], axis=1)

    def norm_half(gg, table):
        for qq in range(nq):
            part, spot = qq // per, qq % per
            m4[part * half : (part + 1) * half, spot * cc : (spot + 1) * cc] = mg[
                gg, qq
            ].astype(F32)
        patch_in = jnp.dot(table, m4[...].astype(BF16), preferred_element_type=F32)
        saved = vout_v[pl.ds(pl.multiple_of(gg * phalf, 16), phalf), :].astype(F32)
        pg = norm_backward(patch_in, saved, scales).astype(BF16)
        pgall[c, gg] = pg
        return pg

    loads["vout"].wait()
    far_g = 1 - g
    near_table, far_table = slot_table(g), slot_table(far_g)
    for d in near_first:
        for e in (1, 0) if d else (1,):
            qq = zrel(d) * 2 + y + e - 2 * y * e
            arrive(mg.at[g, qq], mg_sem.at[qq])
            remote(mg.at[g, qq], mg.at[g, qq], mgx_sem.at[qq], x_peer).start()
    fc2_y(2)
    zh = nz // 2
    cuts = [(0, first_lanes), (first_lanes, fhalf - first_lanes)]

    def piece(i, j, side, k):
        lane = pl.multiple_of(side * fhalf + cuts[k][0], 128)
        return pgall.at[i, j, :, pl.ds(lane, cuts[k][1])]

    def to_core(j, k, which):
        at = piece(c, j, 1 - c, k)
        remote(at, at, pgc_sem.at[k, which], c_peer).start()

    pg_out[...] = norm_half(g, near_table)
    for k in range(2):
        to_core(g, k, 0)
    for qq in range(nq):
        arrive(mg.at[far_g, qq], mgx_sem.at[qq])
    norm_half(far_g, far_table)
    for k in range(2):
        to_core(far_g, k, 1)
    fc2_core(0)
    fc2_core(1)
    fc2_core(3)
    arrive(act.at[1 - c], xw_sem.at[2])
    quarter = 2 * fw
    acts = act.reshape(2 * pslot, hid)
    sent = 0
    for k in range(2):
        arrive(piece(1 - c, g, c, k), pgc_sem.at[k, 0])
        arrive(piece(1 - c, 1 - g, c, k), pgc_sem.at[k, 1])
        begin, size = cuts[k]
        lhs = jnp.concatenate(
            [piece(i, j, c, k)[...] for i in range(2) for j in range(2)], axis=0
        )
        ready = zh if k else (begin + size) // (2 * quarter)
        for hf in range(2):
            col = slice(hf * hh, (hf + 1) * hh)
            own3[begin : begin + size, col] = lax.dot_general(
                lhs, acts[:, col], (((0,), (0,)), ((), ())), preferred_element_type=F32
            )
            for zz in range(sent, ready):
                base = pl.multiple_of((zz * 2 + 1 - y) * quarter, 16)
                for c2 in range(2):
                    kk = zz * 2 + c2
                    y3s[hf, kk] = own3[pl.ds(base + c2 * fw, fw), col].astype(BF16)
                    remote(
                        y3s.at[hf, kk], ry3.at[hf, kk], ry3_sem.at[hf, kk], y_peer
                    ).start()
        sent = ready
    for zz in range(zh):
        base = pl.multiple_of((zz * 2 + y) * quarter, 16)
        for hf in range(2):
            col = slice(hf * hh, (hf + 1) * hh)
            for c2 in range(2):
                k = zz * 2 + c2
                arrive(ry3.at[hf, k], ry3_sem.at[hf, k])
                total = own3[pl.ds(base + c2 * fw, fw), col] + ry3[hf, k].astype(F32)
                to_z = c * zh + zz
                me = (to_z == z) & (c2 == c)
                z3s[hf, k] = total.astype(BF16)

                @pl.when(me)
                def _():
                    rz3[z, hf] = total.astype(BF16)

                unless(
                    me,
                    remote(
                        z3s.at[hf, k],
                        rz3.at[z, hf],
                        rz3_sem.at[z, hf],
                        dev(g, to_z, y, c2),
                    ),
                )

    fc2_core(2)
    for d in range(nz):
        for e in range(2):
            yy = y + e - 2 * y * e
            arrive(fc2_block(zrel(d), yy, 1 - c), fc_sem.at[e, d])
    own_pg = jnp.concatenate([pgall[c, 0], pgall[c, 1]], axis=0)
    wfull = wf.reshape(vit, hid)

    @pl.loop(0, hid // nt)
    def _(t):
        sl = pl.ds(pl.multiple_of(t * nt, nt), nt)
        got = jnp.dot(own_pg, wfull[:, sl], preferred_element_type=F32)
        fc1_out[:, sl] = (fslope[:, sl] * got).astype(BF16)

    for hf in range(2):
        total = jnp.zeros((fw, hh), F32)
        for zz in range(nz):

            @pl.when(jnp.logical_not((zz == z) & (c == z // zh)))
            def _():
                arrive(rz3.at[zz, hf], rz3_sem.at[zz, hf])

            total = total + rz3[zz, hf].astype(F32)
        wg_out[:, hf * hh : (hf + 1) * hh] = total

    for item in sends:
        if isinstance(item, tuple):
            cp, me = item

            @pl.when(jnp.logical_not(me))
            def _():
                cp.wait_send()

        else:
            item.wait_send()


def in_hbm(x):
    return pltpu.with_memory_space_constraint(x, pltpu.HBM)


def fused_on_device(
    llm_grad,
    image_grid,
    image_owner,
    row_start,
    merger_pre,
    vit_out,
    vit_pre,
    ln_gain,
    merger_out_w,
    merger_in_w,
    vit_fc2_w,
    *,
    n_grp,
    n_seq,
):
    n_img = image_owner.shape[0]
    tok, feat = llm_grad.shape
    kb, hid = merger_out_w.shape
    cw = merger_in_w.shape[1]
    pslot, _, vit = vit_out.shape
    fw = vit_fc2_w.shape[0]
    rows = merger_pre.shape[0]
    half, phalf = rows // 2, pslot // 2
    nz, nq, kc, cc = n_seq // 4, n_seq // 2, 2 * kb, 2 * cw
    qg = feat // kc
    vmem, anyspace = pltpu.VMEM, pl.BlockSpec(memory_space=pltpu.HBM)
    vspec = pl.BlockSpec(memory_space=pltpu.VMEM)
    dma = pltpu.SemaphoreType.DMA
    scratch = [
        vmem((2, n_img), jnp.int32),
        vmem((1, n_img), jnp.int32),
        vmem((1, n_img), jnp.int32),
        vmem((vit // 128, 128), F32),
        vmem((tok, feat), BF16),
        vmem((rows, hid), BF16),
        vmem((pslot, vit), BF16),
        vmem((pslot, hid), BF16),
        vmem((kc, hid), BF16),
        vmem((cc, hid), BF16),
        vmem((n_seq, fw, hid), BF16),
        vmem((2, pslot, hid), BF16),
        vmem((pslot, hid), F32),
        vmem((rows, hid), F32),
        vmem((qg, 2, half, kc), BF16),
        vmem((qg, half, kc), BF16),
        vmem((n_seq, half, kc), BF16),
        vmem((n_seq * half, kc), F32),
        vmem((n_seq * half, kc), BF16),
        vmem((2, nz, rows, hid // 2), BF16),
        vmem((2, nz, rows, hid // 2), F32),
        vmem((2, nz, rows, hid // 2), BF16),
        vmem((2, nz, rows, hid // 2), BF16),
        vmem((2, nz, rows, hid // 2), BF16),
        vmem((2, nq, rows, hid // 2), BF16),
        vmem((2 * rows, cc), F32),
        vmem((nz, 2, half, cc), BF16),
        vmem((nz, 2, half, cc), BF16),
        vmem((nz, 2, half, cc), BF16),
        vmem((nz, 2, half, cc), BF16),
        vmem((2, nq, half, cc), BF16),
        vmem((phalf, vit), F32),
        vmem((2, 2, phalf, vit), BF16),
        vmem((vit // 2, hid), F32),
        vmem((2, nz, fw, hid // 2), BF16),
        vmem((2, nz, fw, hid // 2), BF16),
        vmem((2, nz, fw, hid // 2), BF16),
        vmem((nz, 2, fw, hid // 2), BF16),
        dma((qg + 10,)),
        dma((320,)),
        dma((3,)),
        dma((qg,)),
        dma((n_seq,)),
        dma((2, nz)),
        dma((2, nz)),
        dma((2, nz)),
        dma((2, nz)),
        dma((nz,)),
        dma((nq,)),
        dma((nz,)),
        dma((nz,)),
        dma((2, nz)),
        dma((nq,)),
        dma((2, 2)),
        dma((2, nz)),
        dma((nz, 2)),
    ]
    pg, fc1, wg = pl.pallas_call(
        functools.partial(fused_kernel, n_grp, n_seq),
        out_shape=(
            jax.ShapeDtypeStruct((phalf, vit), BF16),
            jax.ShapeDtypeStruct((pslot, hid), BF16),
            jax.ShapeDtypeStruct((fw, hid), F32),
        ),
        in_specs=[anyspace] * 11,
        out_specs=(vspec, vspec, vspec),
        scratch_shapes=scratch,
        compiler_params=pltpu.CompilerParams(
            collective_id=0, has_side_effects=True, vmem_limit_bytes=40 * 1024 * 1024
        ),
    )(
        in_hbm(llm_grad),
        in_hbm(image_grid.T),
        in_hbm(image_owner.reshape(1, n_img)),
        in_hbm(row_start.reshape(1, n_img)),
        in_hbm(merger_pre.reshape(rows, hid)),
        in_hbm(vit_out.reshape(pslot, vit)),
        in_hbm(vit_pre.reshape(pslot, hid)),
        in_hbm(ln_gain.reshape(vit // 128, 128)),
        in_hbm(merger_out_w),
        in_hbm(merger_in_w.T),
        in_hbm(vit_fc2_w),
    )
    return pg.reshape(phalf, 1, vit), fc1.reshape(pslot, 1, hid), wg


def solution(mesh):
    n_grp, n_seq = mesh.shape["grp"], mesh.shape["seq"]

    def step(*args):
        llm_grad, merger_pre, vit_out = args[0], args[4], args[5]
        merger_out_w, merger_in_w, vit_fc2_w = args[8], args[9], args[10]
        feat, (kb, hid), cw = llm_grad.shape[1], merger_out_w.shape, merger_in_w.shape[1]
        vit, fw, rows = vit_out.shape[2], vit_fc2_w.shape[0], merger_pre.shape[0]
        fits = (
            n_grp == 2
            and n_seq >= 8
            and n_seq & (n_seq - 1) == 0
            and feat % (2 * kb) == 0
            and kb % 128 == 0
            and hid % 256 == 0
            and (2 * cw) % 128 == 0
            and vit % (2 * cw) == 0
            and vit % 256 == 0
            and fw % 16 == 0
            and rows == n_seq * SLOT
            and rows % 16 == 0
        )
        if fits:
            return fused_on_device(*args, n_grp=n_grp, n_seq=n_seq)
        return on_device(*args)

    return jax.shard_map(
        step,
        mesh=mesh,
        in_specs=(
            P("seq", "grp"),
            P(),
            P(),
            P(),
            P(None, "seq", "grp"),
            P(None, "seq", None),
            P(None, "seq", "grp"),
            P(),
            P("seq", "grp"),
            P("grp", "seq"),
            P("seq", "grp"),
        ),
        out_specs=(P("grp", "seq", None), P(None, "seq", "grp"), P("seq", "grp")),
        check_vma=False,
    )
```

```python
import functools

import jax
import jax.numpy as jnp
from jax import lax
from jax.experimental import pallas as pl
from jax.experimental.pallas import tpu as pltpu
from jax.sharding import PartitionSpec as P

SLOT = 3
MESH = pl.DeviceIdType.MESH
F32 = jnp.float32
BF16 = jnp.bfloat16


def gelu_slope(values):
    return (
        0.5 * (1.0 + lax.erf(values * 0.7071067811865476))
        + values * jnp.exp(-0.5 * values * values) * 0.3989422804014327
    )


def patch_table(widths, counts, slots):
    places = jnp.arange(4 * slots, dtype=jnp.int32)
    merged = places // 4
    corner = places % 4
    row_in = merged[None, :] // widths[:, None]
    col_in = merged[None, :] % widths[:, None]
    target = (
        (2 * row_in + corner[None, :] // 2) * (2 * widths[:, None])
        + 2 * col_in
        + corner[None, :] % 2
    )
    usable = merged[None, :] < counts[:, None]
    return ((target[:, None, :] == places[None, :, None]) & usable[:, None, :]).astype(jnp.float32)


def norm_backward(upstream, inputs, scales):
    average = jnp.mean(inputs, -1, keepdims=True)
    centred = inputs - average
    inverse_std = lax.rsqrt(jnp.mean(centred * centred, -1, keepdims=True) + 1e-06)
    normed = centred * inverse_std
    scaled = upstream * scales
    return inverse_std * (
        scaled
        - jnp.mean(scaled, -1, keepdims=True)
        - normed * jnp.mean(scaled * normed, -1, keepdims=True)
    )


def on_device(
    llm_grad,
    image_grid,
    image_owner,
    row_start,
    merger_pre,
    vit_out,
    vit_pre,
    ln_gain,
    merger_out_w,
    merger_in_w,
    vit_fc2_w,
):
    seq_count = lax.axis_size("seq")
    own_index = lax.axis_index("seq")
    grids = image_grid.reshape(seq_count, seq_count, 2)
    counts = grids[:, :, 0] * grids[:, :, 1]
    widths = grids[:, :, 1]
    owners = image_owner.reshape(seq_count, seq_count)
    starts = row_start.reshape(seq_count, seq_count)
    within = jnp.arange(SLOT, dtype=jnp.int32)
    peers = jnp.arange(seq_count, dtype=jnp.int32)
    shard_rows = llm_grad.shape[0]
    my_owners = lax.dynamic_index_in_dim(owners, own_index, 0, keepdims=False)
    my_counts = lax.dynamic_index_in_dim(counts, own_index, 0, keepdims=False)
    my_starts = lax.dynamic_index_in_dim(starts, own_index, 0, keepdims=False)
    targets = (my_owners[None, :] == peers[:, None]).astype(jnp.int32)
    send_counts = jnp.sum(targets * my_counts[None, :], 1)
    send_starts = jnp.sum(targets * my_starts[None, :], 1)
    indices = jnp.minimum(send_starts[:, None] + within[None, :], shard_rows - 1)
    usable = within[None, :] < send_counts[:, None]
    picked = jnp.take(llm_grad, indices.reshape(-1), axis=0)
    outgoing = jnp.where(usable.reshape(-1, 1), picked, jnp.zeros_like(picked)).reshape(
        seq_count, SLOT, llm_grad.shape[1]
    )
    received = (owners == own_index).astype(jnp.int32)
    recv_counts = jnp.sum(received * counts, 1)
    recv_widths = jnp.sum(received * widths, 1)
    wide_rows = lax.all_gather(
        outgoing.reshape(-1, llm_grad.shape[1]), "grp", axis=1, tiled=True
    )
    sliced = lax.all_to_all(wide_rows, "seq", split_axis=1, concat_axis=0, tiled=True)
    features = sliced.shape[1]
    by_owner = jnp.swapaxes(
        sliced.reshape(seq_count, seq_count, SLOT, features), 0, 1
    ).reshape(-1, features)
    folded = jnp.dot(by_owner, merger_out_w, preferred_element_type=jnp.float32)
    arrived = lax.all_to_all(
        folded.astype(jnp.bfloat16), "seq", split_axis=0, concat_axis=0, tiled=True
    )
    unit_grad = jnp.sum(
        arrived.reshape(seq_count, seq_count * SLOT, -1).astype(jnp.float32), 0
    ).astype(jnp.bfloat16)
    pre_act = merger_pre[:, 0, :].astype(jnp.float32)
    pre_grad = (gelu_slope(pre_act) * unit_grad.astype(jnp.float32)).astype(jnp.bfloat16)
    all_pre = lax.all_gather(pre_grad, "seq", axis=0, tiled=True)
    part_cols = jnp.dot(all_pre, merger_in_w, preferred_element_type=jnp.float32)
    part_rows = lax.all_to_all(
        part_cols.astype(jnp.bfloat16), "seq", split_axis=0, concat_axis=1, tiled=True
    )
    merged_part = jnp.sum(
        lax.all_gather(part_rows, "grp", axis=0).astype(jnp.float32), 0
    )
    vit_width = vit_out.shape[2]
    table = patch_table(recv_widths, recv_counts, SLOT)
    patch_in = jnp.einsum(
        "spq,sqc->spc",
        table,
        merged_part.reshape(seq_count, 4 * SLOT, vit_width),
        precision=lax.Precision.HIGHEST,
    ).reshape(-1, vit_width)
    patch_grad = norm_backward(patch_in, vit_out[:, 0, :].astype(jnp.float32), ln_gain).astype(
        jnp.bfloat16
    )
    group_rows = patch_grad.shape[0] // lax.axis_size("grp")
    own_rows = lax.dynamic_slice_in_dim(
        patch_grad, lax.axis_index("grp") * group_rows, group_rows, 0
    )
    act_grad = jnp.dot(
        patch_grad,
        lax.all_gather(vit_fc2_w, "seq", axis=0, tiled=True),
        preferred_element_type=jnp.float32,
    )
    fc_in = vit_pre[:, 0, :].astype(jnp.float32)
    sigmoid_q = jax.nn.sigmoid(1.702 * fc_in)
    activation = (fc_in * sigmoid_q).astype(jnp.bfloat16)
    fc1_grad = ((sigmoid_q + 1.702 * fc_in * sigmoid_q * (1.0 - sigmoid_q)) * act_grad).astype(
        jnp.bfloat16
    )
    weight_part = lax.dot_general(
        patch_grad, activation, (((0,), (0,)), ((), ())), preferred_element_type=jnp.float32
    )
    weight_parts = lax.all_to_all(
        weight_part.astype(jnp.bfloat16), "seq", split_axis=0, concat_axis=0, tiled=True
    )
    weight_grad = jnp.sum(
        weight_parts.reshape(seq_count, -1, weight_part.shape[1]).astype(jnp.float32), 0
    )
    return (
        own_rows.reshape(group_rows, 1, vit_width),
        fc1_grad.reshape(-1, 1, vit_pre.shape[2]),
        weight_grad,
    )


def small_div(values, by):
    return (values * ((65536 + by - 1) // by)) >> 16


def iota(shape, dim):
    return lax.broadcasted_iota(jnp.int32, shape, dim)


def sum_where(mask, values):
    return jnp.sum(jnp.where(mask, values, 0.0), 1, keepdims=True).astype(jnp.int32)


def fused_kernel(
    n_grp,
    n_seq,
    llm,
    grid,
    owner,
    start,
    mpre,
    vout,
    vpre,
    gain,
    wout,
    win,
    fc2,
    pg_out,
    fc1_out,
    wg_out,
    grid_v,
    owner_v,
    start_v,
    gain_v,
    llm_v,
    mpre_v,
    vout_v,
    vpre_v,
    wo,
    wi,
    wf,
    act,
    fslope,
    gslope,
    rows_all,
    relay,
    xin,
    xflat,
    xperm,
    ys,
    own1,
    ry,
    zs,
    rz,
    allp,
    p2,
    xs,
    own2,
    rx,
    a2s,
    mg,
    m4,
    pgall,
    own3,
    y3s,
    ry3,
    z3s,
    rz3,
    ld_sem,
    send_sem,
    xw_sem,
    xag_sem,
    xin_sem,
    ry_sem,
    rz_sem,
    agz_sem,
    agy_sem,
    rx_sem,
    mg_sem,
    fz_sem,
    fy_sem,
    fc_sem,
    mgx_sem,
    pgc_sem,
    ry3_sem,
    rz3_sem,
):
    g = lax.axis_index("grp")
    s = lax.axis_index("seq")
    nz = n_seq // 4
    nq = n_seq // 2
    z = s // 4
    y = (s // 2) % 2
    c = s % 2
    q = z * 2 + y
    rows = n_seq * SLOT
    half = rows // 2
    tok, feat = llm.shape
    kc = 2 * wout.shape[0]
    hid = wout.shape[1]
    cw = win.shape[0]
    cc = 2 * cw
    vit = vout.shape[1]
    pslot = vout.shape[0]
    phalf = pslot // 2
    fw = fc2.shape[0]
    n_img = owner.shape[1]
    qg = feat // kc
    nt = 256
    fhalf = vit // 2
    first_lanes = -(-fhalf // 256) * 128

    def dev(gg, zz, yy, c2):
        return (gg, (zz * 2 + yy) * 2 + c2)

    x_peer = dev(1 - g, z, y, c)
    y_peer = dev(g, z, 1 - y, c)
    c_peer = dev(g, z, y, 1 - c)

    def zrel(d):
        out = z
        for k in range(nz.bit_length() - 1):
            if d >> k & 1:
                out = out + (1 << k) * (1 - 2 * (z // (1 << k) % 2))
        return out

    sends = []

    def remote(src, dst, rsem, device):
        cp = pltpu.make_async_remote_copy(
            src_ref=src,
            dst_ref=dst,
            send_sem=send_sem.at[len(sends)],
            recv_sem=rsem,
            device_id=device,
            device_id_type=MESH,
        )
        sends.append(cp)
        return cp

    def arrive(dst, rsem):
        pltpu.make_async_copy(dst, dst, rsem).wait()

    def fc2_block(zz, yy, cc2):
        return wf.at[dev(g, zz, yy, cc2)[1]]

    def fc2_z(d):
        own = wf.at[s]
        remote(own, own, fz_sem.at[d], dev(g, zrel(d), y, c)).start()

    def fc2_near():
        own = wf.at[s]
        remote(own, own, fy_sem.at[0], y_peer).start()
        remote(own, own, fc_sem.at[0, 0], c_peer).start()

    def fc2_y(d):
        blk = fc2_block(zrel(d), y, c)
        arrive(blk, fz_sem.at[d])
        remote(blk, blk, fy_sem.at[d], y_peer).start()
        remote(blk, blk, fc_sem.at[0, d], c_peer).start()

    def fc2_core(d):
        blk = fc2_block(zrel(d), 1 - y, c)
        arrive(blk, fy_sem.at[d])
        remote(blk, blk, fc_sem.at[1, d], c_peer).start()

    barrier = pltpu.get_barrier_semaphore()

    @pl.loop(0, n_grp * n_seq)
    def _(i):
        @pl.when(i != g * n_seq + s)
        def _():
            pl.semaphore_signal(
                barrier, inc=1, device_id=(i // n_seq, i % n_seq), device_id_type=MESH
            )

    loads = {}

    def load(name, src, dst):
        cp = pltpu.make_async_copy(src, dst, ld_sem.at[len(loads)])
        cp.start()
        loads[name] = cp

    load("grid", grid, grid_v)
    load("owner", owner, owner_v)
    load("start", start, start_v)
    for i in range(qg):
        load(("llm", i), llm.at[:, pl.ds(i * kc, kc)], llm_v.at[:, pl.ds(i * kc, kc)])
    load("gain", gain, gain_v)
    load("vpre", vpre, vpre_v)
    load("mpre", mpre, mpre_v)
    wo_own = wo.at[pl.ds(pl.multiple_of(c * (kc // 2), 16), kc // 2)]
    load("wo", wout, wo_own)
    wi_own = wi.at[pl.ds(pl.multiple_of(c * cw, 16), cw)]
    wi_far = wi.at[pl.ds(pl.multiple_of((1 - c) * cw, 16), cw)]
    load("wi", win, wi_own)
    load("wf", fc2, wf.at[s])
    load("vout", vout, vout_v)

    r = iota((rows, 1), 0)
    par = small_div(r, half)
    rem = r - par * half
    o2 = small_div(rem, SLOT)
    slot = rem - o2 * SLOT
    img = iota((1, n_img), 1)
    for name in ("grid", "owner", "start"):
        loads[name].wait()
    shard_of = small_div(img, n_seq)
    count = (grid_v[0:1, :] * grid_v[1:2, :]).astype(F32)
    width = grid_v[1:2, :].astype(F32)
    starts = start_v[...].astype(F32)
    owners = owner_v[...]
    mine = (owners == o2 * 2 + par) & (shard_of == s)
    first = sum_where(mine, jnp.broadcast_to(starts, mine.shape))
    many = sum_where(mine, jnp.broadcast_to(count, mine.shape))
    onehot = ((iota((rows, tok), 1) == first + slot) & (slot < many)).astype(BF16)

    for i in range(qg):
        loads[("llm", i)].wait()
        picked = jnp.dot(
            onehot, llm_v[:, i * kc : (i + 1) * kc], preferred_element_type=F32
        ).astype(BF16)
        rows_all[i, 0] = picked[:half]
        rows_all[i, 1] = picked[half:]

    pl.semaphore_wait(barrier, n_grp * n_seq - 1)

    for i in range(qg):
        remote(rows_all.at[i, 1], relay.at[i], xag_sem.at[i], x_peer).start()

    def unless(me, cp):
        @pl.when(jnp.logical_not(me))
        def _():
            cp.start()

        sends.pop()
        sends.append((cp, me))

    def send_rows(src, qq, p):
        cp = remote(src, xin.at[s], xin_sem.at[s], (g, qq * 2 + p))
        me = (qq == q) & (p == c)

        @pl.when(me)
        def _():
            pltpu.make_async_copy(src, xin.at[s], xin_sem.at[s]).start()

        unless(me, cp)

    for i in range(qg):
        send_rows(rows_all.at[i, 0], g * qg + i, 0)

    loads["wf"].wait()
    remote(wout, wo_own, xw_sem.at[0], c_peer).start()
    remote(win, wi_own, xw_sem.at[1], c_peer).start()

    for i in range(qg):
        arrive(relay.at[i], xag_sem.at[i])
        send_rows(relay.at[i], (1 - g) * qg + i, 1)

    fc2_z(1)
    fc2_z(3)
    fc2_near()
    loads["vpre"].wait()
    tile = 64 if pslot % 64 == 0 else 16

    @pl.loop(0, pslot // tile)
    def _(i):
        sl = pl.ds(pl.multiple_of(i * tile, tile), tile)
        v = vpre_v[sl, :].astype(F32)
        sq = jax.nn.sigmoid(1.702 * v)
        act[c, sl, :] = (v * sq).astype(BF16)
        fslope[sl, :] = sq + 1.702 * v * sq * (1.0 - sq)

    remote(act.at[c], act.at[c], xw_sem.at[2], c_peer).start()
    loads["mpre"].wait()
    gslope[...] = gelu_slope(mpre_v[...].astype(F32))

    r = iota((half * n_seq, 1), 0)
    oo = small_div(r, rows)
    rem = r - oo * rows
    src_s = small_div(rem, SLOT)
    slot = rem - src_s * SLOT
    yo = small_div(oo, nz)
    zo = oo - yo * nz
    want = src_s * half + (zo * 2 + yo) * SLOT + slot
    perm = (iota((half * n_seq, half * n_seq), 1) == want).astype(BF16)

    loads["gain"].wait()
    loads["wi"].wait()
    arrive(wi_far, xw_sem.at[1])
    loads["wo"].wait()
    arrive(wo.at[pl.ds(pl.multiple_of((1 - c) * (kc // 2), 16), kc // 2)], xw_sem.at[0])

    first_hand = (g + c + q // qg) % 2 == 0
    for d in range(nz):
        for k in range(4):
            src = zrel(d) * 4 + k
            arrive(xin.at[src], xin_sem.at[src])
            unless(
                jnp.logical_not(first_hand),
                remote(xin.at[src], xin.at[src], xin_sem.at[src], x_peer),
            )
            at = pl.ds(pl.multiple_of(src * half, 8), half)
            xflat[at, :] = xin[src].astype(F32)

    @pl.loop(0, kc // nt)
    def _(t):
        sl = pl.ds(pl.multiple_of(t * nt, nt), nt)
        xperm[:, sl] = jnp.dot(
            perm, xflat[:, sl].astype(BF16), preferred_element_type=F32
        ).astype(BF16)

    hrows = nz * rows

    hh = hid // 2
    order = list(range(nz - 1, -1, -1))

    def part1(yy, hf, out):
        lhs = xperm[pl.ds(pl.multiple_of(yy * hrows, 16), hrows), :]
        got = jnp.dot(lhs, wo[:, hf * hh : (hf + 1) * hh], preferred_element_type=F32)
        for zz in range(nz):
            out[hf, zz] = got[zz * rows : (zz + 1) * rows].astype(out.dtype)

    for hf in range(2):
        part1(1 - y, hf, ys)
        for d in order:
            zz = zrel(d)
            remote(ys.at[hf, zz], ry.at[hf, zz], ry_sem.at[hf, d], y_peer).start()
    for hf in range(2):
        part1(y, hf, own1)
    units = {}

    def over_y(hf, d):
        zz = zrel(d)
        arrive(ry.at[hf, zz], ry_sem.at[hf, d])
        total = own1[hf, zz] + ry[hf, zz].astype(F32)
        if d:
            zs[hf, d] = total.astype(BF16)
            remote(zs.at[hf, d], rz.at[hf, d], rz_sem.at[hf, d], dev(g, zz, y, c)).start()
        else:
            units[hf] = total

    def over_z(hf):
        unit = units[hf]
        for d in order[:-1]:
            arrive(rz.at[hf, d], rz_sem.at[hf, d])
            unit = unit + rz[hf, d].astype(F32)
        slope = gslope[:, hf * hh : (hf + 1) * hh]
        allp[hf, q] = (slope * unit.astype(BF16).astype(F32)).astype(BF16)
        mine = allp.at[hf, q]
        remote(mine, mine, agy_sem.at[hf, 0], y_peer).start()
        for d in order[:-1]:
            remote(mine, mine, agz_sem.at[hf, d], dev(g, zrel(d), y, c)).start()

    for d in order:
        over_y(0, d)
    for d in order:
        over_y(1, d)
    over_z(0)
    over_z(1)
    fc2_y(1)
    near_first = [0] + order[:-1]
    for hf in range(2):
        for d in near_first[1:]:
            qq = zrel(d) * 2 + y
            arrive(allp.at[hf, qq], agz_sem.at[hf, d])
            remote(allp.at[hf, qq], allp.at[hf, qq], agy_sem.at[hf, d], y_peer).start()

    fc2_z(2)
    def columns_of(d):
        zz = zrel(d)
        got = jnp.zeros((2 * rows, cc), F32)
        for hf in range(2):
            arrive(allp.at[hf, zz * 2 + 1 - y], agy_sem.at[hf, d])
            got = got + lax.dot_general(
                allp[hf, pl.ds(zz * 2, 2)].reshape(2 * rows, hh),
                wi[:, hf * hh : (hf + 1) * hh],
                (((1,), (1,)), ((), ())),
                preferred_element_type=F32,
            )
        p2[...] = got
        for e in range(2):
            yo = y + e - 2 * y * e
            far = pl.ds(pl.multiple_of(yo * rows + (1 - g) * half, 8), half)
            near = pl.ds(pl.multiple_of(yo * rows + g * half, 8), half)
            xs[d, e] = p2[far, :].astype(BF16)
            own2[d, e] = p2[near, :].astype(BF16)
        remote(xs.at[d], rx.at[d], rx_sem.at[d], x_peer).start()

    def to_owners(d):
        arrive(rx.at[d], rx_sem.at[d])
        for e in (1, 0):
            yo = y + e - 2 * y * e
            total = (own2[d, e].astype(F32) + rx[d, e].astype(F32)).astype(BF16)
            if d == 0 and e == 0:
                mg[g, q] = total
                remote(mg.at[g, q], mg.at[g, q], mgx_sem.at[q], x_peer).start()
            else:
                a2s[d, e] = total
                remote(
                    a2s.at[d, e], mg.at[g, q], mg_sem.at[q], dev(g, zrel(d), yo, c)
                ).start()

    for k, d in enumerate(near_first):
        columns_of(d)
        if k:
            to_owners(near_first[k - 1])
    fc2_y(3)
    to_owners(near_first[-1])
    def slot_table(gg):
        shape = (phalf, phalf)
        r = iota((phalf, 1), 0)
        src_r = small_div(r, 4 * SLOT)
        place = r - src_r * (4 * SLOT)
        mine = (owners == s) & (shard_of == src_r + gg * (n_seq // 2))
        many = sum_where(mine, jnp.broadcast_to(count, mine.shape))
        wide = sum_where(mine, jnp.broadcast_to(width, mine.shape))
        col = iota(shape, 1)
        comp = small_div(col, half)
        rem = col - comp * half
        src_c = small_div(rem, SLOT)
        slot = rem - src_c * SLOT
        row_in = jnp.zeros(shape, jnp.int32)
        for k in range(1, SLOT):
            row_in = row_in + (slot >= k * wide).astype(jnp.int32)
        col_in = slot - row_in * wide
        upper = comp >> 1
        target = (2 * row_in + upper) * (2 * wide) + 2 * col_in + (comp - 2 * upper)
        return ((src_c == src_r) & (slot < many) & (target == place)).astype(BF16)

    per = vit // cc
    scales = jnp.concatenate([gain_v[k : k + 1, :] for k in range(vit // 128)], axis=1)

    def norm_half(gg, table):
        for qq in range(nq):
            part, spot = qq // per, qq % per
            m4[part * half : (part + 1) * half, spot * cc : (spot + 1) * cc] = mg[
                gg, qq
            ].astype(F32)
        patch_in = jnp.dot(table, m4[...].astype(BF16), preferred_element_type=F32)
        saved = vout_v[pl.ds(pl.multiple_of(gg * phalf, 16), phalf), :].astype(F32)
        pg = norm_backward(patch_in, saved, scales).astype(BF16)
        pgall[c, gg] = pg
        return pg

    loads["vout"].wait()
    far_g = 1 - g
    near_table, far_table = slot_table(g), slot_table(far_g)
    for d in near_first:
        for e in (1, 0) if d else (1,):
            qq = zrel(d) * 2 + y + e - 2 * y * e
            arrive(mg.at[g, qq], mg_sem.at[qq])
            remote(mg.at[g, qq], mg.at[g, qq], mgx_sem.at[qq], x_peer).start()
    fc2_y(2)
    zh = nz // 2
    cuts = [(0, first_lanes), (first_lanes, fhalf - first_lanes)]

    def piece(i, j, side, k):
        lane = pl.multiple_of(side * fhalf + cuts[k][0], 128)
        return pgall.at[i, j, :, pl.ds(lane, cuts[k][1])]

    def to_core(j, k, which):
        at = piece(c, j, 1 - c, k)
        remote(at, at, pgc_sem.at[k, which], c_peer).start()

    pg_out[...] = norm_half(g, near_table)
    for k in range(2):
        to_core(g, k, 0)
    for qq in range(nq):
        arrive(mg.at[far_g, qq], mgx_sem.at[qq])
    norm_half(far_g, far_table)
    for k in range(2):
        to_core(far_g, k, 1)
    fc2_core(0)
    fc2_core(1)
    fc2_core(3)
    arrive(act.at[1 - c], xw_sem.at[2])
    quarter = 2 * fw
    acts = act.reshape(2 * pslot, hid)
    sent = 0
    for k in range(2):
        arrive(piece(1 - c, g, c, k), pgc_sem.at[k, 0])
        arrive(piece(1 - c, 1 - g, c, k), pgc_sem.at[k, 1])
        begin, size = cuts[k]
        lhs = jnp.concatenate(
            [piece(i, j, c, k)[...] for i in range(2) for j in range(2)], axis=0
        )
        ready = zh if k else (begin + size) // (2 * quarter)
        for hf in range(2):
            col = slice(hf * hh, (hf + 1) * hh)
            own3[begin : begin + size, col] = lax.dot_general(
                lhs, acts[:, col], (((0,), (0,)), ((), ())), preferred_element_type=F32
            )
            for zz in range(sent, ready):
                base = pl.multiple_of((zz * 2 + 1 - y) * quarter, 16)
                for c2 in range(2):
                    kk = zz * 2 + c2
                    y3s[hf, kk] = own3[pl.ds(base + c2 * fw, fw), col].astype(BF16)
                    remote(
                        y3s.at[hf, kk], ry3.at[hf, kk], ry3_sem.at[hf, kk], y_peer
                    ).start()
        sent = ready
    for zz in range(zh):
        base = pl.multiple_of((zz * 2 + y) * quarter, 16)
        for hf in range(2):
            col = slice(hf * hh, (hf + 1) * hh)
            for c2 in range(2):
                k = zz * 2 + c2
                arrive(ry3.at[hf, k], ry3_sem.at[hf, k])
                total = own3[pl.ds(base + c2 * fw, fw), col] + ry3[hf, k].astype(F32)
                to_z = c * zh + zz
                me = (to_z == z) & (c2 == c)
                z3s[hf, k] = total.astype(BF16)

                @pl.when(me)
                def _():
                    rz3[z, hf] = total.astype(BF16)

                unless(
                    me,
                    remote(
                        z3s.at[hf, k],
                        rz3.at[z, hf],
                        rz3_sem.at[z, hf],
                        dev(g, to_z, y, c2),
                    ),
                )

    fc2_core(2)
    for d in range(nz):
        for e in range(2):
            yy = y + e - 2 * y * e
            arrive(fc2_block(zrel(d), yy, 1 - c), fc_sem.at[e, d])
    own_pg = jnp.concatenate([pgall[c, 0], pgall[c, 1]], axis=0)
    wfull = wf.reshape(vit, hid)

    @pl.loop(0, hid // nt)
    def _(t):
        sl = pl.ds(pl.multiple_of(t * nt, nt), nt)
        got = jnp.dot(own_pg, wfull[:, sl], preferred_element_type=F32)
        fc1_out[:, sl] = (fslope[:, sl] * got).astype(BF16)

    for hf in range(2):
        total = jnp.zeros((fw, hh), F32)
        for zz in range(nz):

            @pl.when(jnp.logical_not((zz == z) & (c == z // zh)))
            def _():
                arrive(rz3.at[zz, hf], rz3_sem.at[zz, hf])

            total = total + rz3[zz, hf].astype(F32)
        wg_out[:, hf * hh : (hf + 1) * hh] = total

    for item in sends:
        if isinstance(item, tuple):
            cp, me = item

            @pl.when(jnp.logical_not(me))
            def _():
                cp.wait_send()

        else:
            item.wait_send()


def in_hbm(x):
    return pltpu.with_memory_space_constraint(x, pltpu.HBM)


def fused_on_device(
    llm_grad,
    image_grid,
    image_owner,
    row_start,
    merger_pre,
    vit_out,
    vit_pre,
    ln_gain,
    merger_out_w,
    merger_in_w,
    vit_fc2_w,
    *,
    n_grp,
    n_seq,
):
    n_img = image_owner.shape[0]
    tok, feat = llm_grad.shape
    kb, hid = merger_out_w.shape
    cw = merger_in_w.shape[1]
    pslot, _, vit = vit_out.shape
    fw = vit_fc2_w.shape[0]
    rows = merger_pre.shape[0]
    half, phalf = rows // 2, pslot // 2
    nz, nq, kc, cc = n_seq // 4, n_seq // 2, 2 * kb, 2 * cw
    qg = feat // kc
    vmem, anyspace = pltpu.VMEM, pl.BlockSpec(memory_space=pltpu.HBM)
    vspec = pl.BlockSpec(memory_space=pltpu.VMEM)
    dma = pltpu.SemaphoreType.DMA
    scratch = [
        vmem((2, n_img), jnp.int32),
        vmem((1, n_img), jnp.int32),
        vmem((1, n_img), jnp.int32),
        vmem((vit // 128, 128), F32),
        vmem((tok, feat), BF16),
        vmem((rows, hid), BF16),
        vmem((pslot, vit), BF16),
        vmem((pslot, hid), BF16),
        vmem((kc, hid), BF16),
        vmem((cc, hid), BF16),
        vmem((n_seq, fw, hid), BF16),
        vmem((2, pslot, hid), BF16),
        vmem((pslot, hid), F32),
        vmem((rows, hid), F32),
        vmem((qg, 2, half, kc), BF16),
        vmem((qg, half, kc), BF16),
        vmem((n_seq, half, kc), BF16),
        vmem((n_seq * half, kc), F32),
        vmem((n_seq * half, kc), BF16),
        vmem((2, nz, rows, hid // 2), BF16),
        vmem((2, nz, rows, hid // 2), F32),
        vmem((2, nz, rows, hid // 2), BF16),
        vmem((2, nz, rows, hid // 2), BF16),
        vmem((2, nz, rows, hid // 2), BF16),
        vmem((2, nq, rows, hid // 2), BF16),
        vmem((2 * rows, cc), F32),
        vmem((nz, 2, half, cc), BF16),
        vmem((nz, 2, half, cc), BF16),
        vmem((nz, 2, half, cc), BF16),
        vmem((nz, 2, half, cc), BF16),
        vmem((2, nq, half, cc), BF16),
        vmem((phalf, vit), F32),
        vmem((2, 2, phalf, vit), BF16),
        vmem((vit // 2, hid), F32),
        vmem((2, nz, fw, hid // 2), BF16),
        vmem((2, nz, fw, hid // 2), BF16),
        vmem((2, nz, fw, hid // 2), BF16),
        vmem((nz, 2, fw, hid // 2), BF16),
        dma((qg + 10,)),
        dma((320,)),
        dma((3,)),
        dma((qg,)),
        dma((n_seq,)),
        dma((2, nz)),
        dma((2, nz)),
        dma((2, nz)),
        dma((2, nz)),
        dma((nz,)),
        dma((nq,)),
        dma((nz,)),
        dma((nz,)),
        dma((2, nz)),
        dma((nq,)),
        dma((2, 2)),
        dma((2, nz)),
        dma((nz, 2)),
    ]
    pg, fc1, wg = pl.pallas_call(
        functools.partial(fused_kernel, n_grp, n_seq),
        out_shape=(
            jax.ShapeDtypeStruct((phalf, vit), BF16),
            jax.ShapeDtypeStruct((pslot, hid), BF16),
            jax.ShapeDtypeStruct((fw, hid), F32),
        ),
        in_specs=[anyspace] * 11,
        out_specs=(vspec, vspec, vspec),
        scratch_shapes=scratch,
        compiler_params=pltpu.CompilerParams(
            collective_id=0, has_side_effects=True, vmem_limit_bytes=40 * 1024 * 1024
        ),
    )(
        in_hbm(llm_grad),
        in_hbm(image_grid.T),
        in_hbm(image_owner.reshape(1, n_img)),
        in_hbm(row_start.reshape(1, n_img)),
        in_hbm(merger_pre.reshape(rows, hid)),
        in_hbm(vit_out.reshape(pslot, vit)),
        in_hbm(vit_pre.reshape(pslot, hid)),
        in_hbm(ln_gain.reshape(vit // 128, 128)),
        in_hbm(merger_out_w),
        in_hbm(merger_in_w.T),
        in_hbm(vit_fc2_w),
    )
    return pg.reshape(phalf, 1, vit), fc1.reshape(pslot, 1, hid), wg


def solution(mesh):
    n_grp, n_seq = mesh.shape["grp"], mesh.shape["seq"]

    def step(*args):
        llm_grad, merger_pre, vit_out = args[0], args[4], args[5]
        merger_out_w, merger_in_w, vit_fc2_w = args[8], args[9], args[10]
        feat, (kb, hid), cw = llm_grad.shape[1], merger_out_w.shape, merger_in_w.shape[1]
        vit, fw, rows = vit_out.shape[2], vit_fc2_w.shape[0], merger_pre.shape[0]
        fits = (
            n_grp == 2
            and n_seq >= 8
            and n_seq & (n_seq - 1) == 0
            and feat % (2 * kb) == 0
            and kb % 128 == 0
            and hid % 256 == 0
            and (2 * cw) % 128 == 0
            and vit % (2 * cw) == 0
            and vit % 256 == 0
            and fw % 16 == 0
            and rows == n_seq * SLOT
            and rows % 16 == 0
        )
        if fits:
            return fused_on_device(*args, n_grp=n_grp, n_seq=n_seq)
        return on_device(*args)

    return jax.shard_map(
        step,
        mesh=mesh,
        in_specs=(
            P("seq", "grp"),
            P(),
            P(),
            P(),
            P(None, "seq", "grp"),
            P(None, "seq", None),
            P(None, "seq", "grp"),
            P(),
            P("seq", "grp"),
            P("grp", "seq"),
            P("seq", "grp"),
        ),
        out_specs=(P("grp", "seq", None), P(None, "seq", "grp"), P("seq", "grp")),
        check_vma=False,
    )
```

```python
import functools

import jax
import jax.numpy as jnp
from jax import lax
from jax.experimental import pallas as pl
from jax.experimental.pallas import tpu as pltpu
from jax.sharding import PartitionSpec as P

SLOT = 3
MESH = pl.DeviceIdType.MESH
F32 = jnp.float32
BF16 = jnp.bfloat16


def gelu_slope(values):
    return (
        0.5 * (1.0 + lax.erf(values * 0.7071067811865476))
        + values * jnp.exp(-0.5 * values * values) * 0.3989422804014327
    )


def patch_table(widths, counts, slots):
    places = jnp.arange(4 * slots, dtype=jnp.int32)
    merged = places // 4
    corner = places % 4
    row_in = merged[None, :] // widths[:, None]
    col_in = merged[None, :] % widths[:, None]
    target = (
        (2 * row_in + corner[None, :] // 2) * (2 * widths[:, None])
        + 2 * col_in
        + corner[None, :] % 2
    )
    usable = merged[None, :] < counts[:, None]
    return ((target[:, None, :] == places[None, :, None]) & usable[:, None, :]).astype(jnp.float32)


def norm_backward(upstream, inputs, scales):
    average = jnp.mean(inputs, -1, keepdims=True)
    centred = inputs - average
    inverse_std = lax.rsqrt(jnp.mean(centred * centred, -1, keepdims=True) + 1e-06)
    normed = centred * inverse_std
    scaled = upstream * scales
    return inverse_std * (
        scaled
        - jnp.mean(scaled, -1, keepdims=True)
        - normed * jnp.mean(scaled * normed, -1, keepdims=True)
    )


def on_device(
    llm_grad,
    image_grid,
    image_owner,
    row_start,
    merger_pre,
    vit_out,
    vit_pre,
    ln_gain,
    merger_out_w,
    merger_in_w,
    vit_fc2_w,
):
    seq_count = lax.axis_size("seq")
    own_index = lax.axis_index("seq")
    grids = image_grid.reshape(seq_count, seq_count, 2)
    counts = grids[:, :, 0] * grids[:, :, 1]
    widths = grids[:, :, 1]
    owners = image_owner.reshape(seq_count, seq_count)
    starts = row_start.reshape(seq_count, seq_count)
    within = jnp.arange(SLOT, dtype=jnp.int32)
    peers = jnp.arange(seq_count, dtype=jnp.int32)
    shard_rows = llm_grad.shape[0]
    my_owners = lax.dynamic_index_in_dim(owners, own_index, 0, keepdims=False)
    my_counts = lax.dynamic_index_in_dim(counts, own_index, 0, keepdims=False)
    my_starts = lax.dynamic_index_in_dim(starts, own_index, 0, keepdims=False)
    targets = (my_owners[None, :] == peers[:, None]).astype(jnp.int32)
    send_counts = jnp.sum(targets * my_counts[None, :], 1)
    send_starts = jnp.sum(targets * my_starts[None, :], 1)
    indices = jnp.minimum(send_starts[:, None] + within[None, :], shard_rows - 1)
    usable = within[None, :] < send_counts[:, None]
    picked = jnp.take(llm_grad, indices.reshape(-1), axis=0)
    outgoing = jnp.where(usable.reshape(-1, 1), picked, jnp.zeros_like(picked)).reshape(
        seq_count, SLOT, llm_grad.shape[1]
    )
    received = (owners == own_index).astype(jnp.int32)
    recv_counts = jnp.sum(received * counts, 1)
    recv_widths = jnp.sum(received * widths, 1)
    wide_rows = lax.all_gather(
        outgoing.reshape(-1, llm_grad.shape[1]), "grp", axis=1, tiled=True
    )
    sliced = lax.all_to_all(wide_rows, "seq", split_axis=1, concat_axis=0, tiled=True)
    features = sliced.shape[1]
    by_owner = jnp.swapaxes(
        sliced.reshape(seq_count, seq_count, SLOT, features), 0, 1
    ).reshape(-1, features)
    folded = jnp.dot(by_owner, merger_out_w, preferred_element_type=jnp.float32)
    arrived = lax.all_to_all(
        folded.astype(jnp.bfloat16), "seq", split_axis=0, concat_axis=0, tiled=True
    )
    unit_grad = jnp.sum(
        arrived.reshape(seq_count, seq_count * SLOT, -1).astype(jnp.float32), 0
    ).astype(jnp.bfloat16)
    pre_act = merger_pre[:, 0, :].astype(jnp.float32)
    pre_grad = (gelu_slope(pre_act) * unit_grad.astype(jnp.float32)).astype(jnp.bfloat16)
    all_pre = lax.all_gather(pre_grad, "seq", axis=0, tiled=True)
    part_cols = jnp.dot(all_pre, merger_in_w, preferred_element_type=jnp.float32)
    part_rows = lax.all_to_all(
        part_cols.astype(jnp.bfloat16), "seq", split_axis=0, concat_axis=1, tiled=True
    )
    merged_part = jnp.sum(
        lax.all_gather(part_rows, "grp", axis=0).astype(jnp.float32), 0
    )
    vit_width = vit_out.shape[2]
    table = patch_table(recv_widths, recv_counts, SLOT)
    patch_in = jnp.einsum(
        "spq,sqc->spc",
        table,
        merged_part.reshape(seq_count, 4 * SLOT, vit_width),
        precision=lax.Precision.HIGHEST,
    ).reshape(-1, vit_width)
    patch_grad = norm_backward(patch_in, vit_out[:, 0, :].astype(jnp.float32), ln_gain).astype(
        jnp.bfloat16
    )
    group_rows = patch_grad.shape[0] // lax.axis_size("grp")
    own_rows = lax.dynamic_slice_in_dim(
        patch_grad, lax.axis_index("grp") * group_rows, group_rows, 0
    )
    act_grad = jnp.dot(
        patch_grad,
        lax.all_gather(vit_fc2_w, "seq", axis=0, tiled=True),
        preferred_element_type=jnp.float32,
    )
    fc_in = vit_pre[:, 0, :].astype(jnp.float32)
    sigmoid_q = jax.nn.sigmoid(1.702 * fc_in)
    activation = (fc_in * sigmoid_q).astype(jnp.bfloat16)
    fc1_grad = ((sigmoid_q + 1.702 * fc_in * sigmoid_q * (1.0 - sigmoid_q)) * act_grad).astype(
        jnp.bfloat16
    )
    weight_part = lax.dot_general(
        patch_grad, activation, (((0,), (0,)), ((), ())), preferred_element_type=jnp.float32
    )
    weight_parts = lax.all_to_all(
        weight_part.astype(jnp.bfloat16), "seq", split_axis=0, concat_axis=0, tiled=True
    )
    weight_grad = jnp.sum(
        weight_parts.reshape(seq_count, -1, weight_part.shape[1]).astype(jnp.float32), 0
    )
    return (
        own_rows.reshape(group_rows, 1, vit_width),
        fc1_grad.reshape(-1, 1, vit_pre.shape[2]),
        weight_grad,
    )


def small_div(values, by):
    return (values * ((65536 + by - 1) // by)) >> 16


def iota(shape, dim):
    return lax.broadcasted_iota(jnp.int32, shape, dim)


def sum_where(mask, values):
    return jnp.sum(jnp.where(mask, values, 0.0), 1, keepdims=True).astype(jnp.int32)


def fused_kernel(
    n_grp,
    n_seq,
    llm,
    grid,
    owner,
    start,
    mpre,
    vout,
    vpre,
    gain,
    wout,
    win,
    fc2,
    pg_out,
    fc1_out,
    wg_out,
    grid_v,
    owner_v,
    start_v,
    gain_v,
    llm_v,
    mpre_v,
    vout_v,
    vpre_v,
    wo,
    wi,
    wf,
    act,
    fslope,
    gslope,
    rows_all,
    relay,
    xin,
    xflat,
    xperm,
    ys,
    own1,
    ry,
    zs,
    rz,
    allp,
    p2,
    xs,
    own2,
    rx,
    a2s,
    mg,
    m4,
    pgall,
    own3,
    y3s,
    ry3,
    z3s,
    rz3,
    ld_sem,
    send_sem,
    xw_sem,
    xag_sem,
    xin_sem,
    ry_sem,
    rz_sem,
    agz_sem,
    agy_sem,
    rx_sem,
    mg_sem,
    fz_sem,
    fy_sem,
    fc_sem,
    mgx_sem,
    pgc_sem,
    ry3_sem,
    rz3_sem,
):
    g = lax.axis_index("grp")
    s = lax.axis_index("seq")
    nz = n_seq // 4
    nq = n_seq // 2
    z = s // 4
    y = (s // 2) % 2
    c = s % 2
    q = z * 2 + y
    rows = n_seq * SLOT
    half = rows // 2
    tok, feat = llm.shape
    kc = 2 * wout.shape[0]
    hid = wout.shape[1]
    cw = win.shape[0]
    cc = 2 * cw
    vit = vout.shape[1]
    pslot = vout.shape[0]
    phalf = pslot // 2
    fw = fc2.shape[0]
    n_img = owner.shape[1]
    qg = feat // kc
    nt = 256
    fhalf = vit // 2
    first_lanes = -(-fhalf // 256) * 128

    def dev(gg, zz, yy, c2):
        return (gg, (zz * 2 + yy) * 2 + c2)

    x_peer = dev(1 - g, z, y, c)
    y_peer = dev(g, z, 1 - y, c)
    c_peer = dev(g, z, y, 1 - c)

    def zrel(d):
        out = z
        for k in range(nz.bit_length() - 1):
            if d >> k & 1:
                out = out + (1 << k) * (1 - 2 * (z // (1 << k) % 2))
        return out

    sends = []

    def remote(src, dst, rsem, device):
        cp = pltpu.make_async_remote_copy(
            src_ref=src,
            dst_ref=dst,
            send_sem=send_sem.at[len(sends)],
            recv_sem=rsem,
            device_id=device,
            device_id_type=MESH,
        )
        sends.append(cp)
        return cp

    def arrive(dst, rsem):
        pltpu.make_async_copy(dst, dst, rsem).wait()

    def fc2_block(zz, yy, cc2):
        return wf.at[dev(g, zz, yy, cc2)[1]]

    def fc2_z(d):
        own = wf.at[s]
        remote(own, own, fz_sem.at[d], dev(g, zrel(d), y, c)).start()

    def fc2_near():
        own = wf.at[s]
        remote(own, own, fy_sem.at[0], y_peer).start()
        remote(own, own, fc_sem.at[0, 0], c_peer).start()

    def fc2_y(d):
        blk = fc2_block(zrel(d), y, c)
        arrive(blk, fz_sem.at[d])
        remote(blk, blk, fy_sem.at[d], y_peer).start()
        remote(blk, blk, fc_sem.at[0, d], c_peer).start()

    def fc2_core(d):
        blk = fc2_block(zrel(d), 1 - y, c)
        arrive(blk, fy_sem.at[d])
        remote(blk, blk, fc_sem.at[1, d], c_peer).start()

    barrier = pltpu.get_barrier_semaphore()

    @pl.loop(0, n_grp * n_seq)
    def _(i):
        @pl.when(i != g * n_seq + s)
        def _():
            pl.semaphore_signal(
                barrier, inc=1, device_id=(i // n_seq, i % n_seq), device_id_type=MESH
            )

    loads = {}

    def load(name, src, dst):
        cp = pltpu.make_async_copy(src, dst, ld_sem.at[len(loads)])
        cp.start()
        loads[name] = cp

    load("grid", grid, grid_v)
    load("owner", owner, owner_v)
    load("start", start, start_v)
    for i in range(qg):
        load(("llm", i), llm.at[:, pl.ds(i * kc, kc)], llm_v.at[:, pl.ds(i * kc, kc)])
    load("gain", gain, gain_v)
    load("vpre", vpre, vpre_v)
    load("mpre", mpre, mpre_v)
    wo_own = wo.at[pl.ds(pl.multiple_of(c * (kc // 2), 16), kc // 2)]
    load("wo", wout, wo_own)
    wi_own = wi.at[pl.ds(pl.multiple_of(c * cw, 16), cw)]
    wi_far = wi.at[pl.ds(pl.multiple_of((1 - c) * cw, 16), cw)]
    load("wi", win, wi_own)
    load("wf", fc2, wf.at[s])
    load("vout", vout, vout_v)

    r = iota((rows, 1), 0)
    par = small_div(r, half)
    rem = r - par * half
    o2 = small_div(rem, SLOT)
    slot = rem - o2 * SLOT
    img = iota((1, n_img), 1)
    for name in ("grid", "owner", "start"):
        loads[name].wait()
    shard_of = small_div(img, n_seq)
    count = (grid_v[0:1, :] * grid_v[1:2, :]).astype(F32)
    width = grid_v[1:2, :].astype(F32)
    starts = start_v[...].astype(F32)
    owners = owner_v[...]
    mine = (owners == o2 * 2 + par) & (shard_of == s)
    first = sum_where(mine, jnp.broadcast_to(starts, mine.shape))
    many = sum_where(mine, jnp.broadcast_to(count, mine.shape))
    onehot = ((iota((rows, tok), 1) == first + slot) & (slot < many)).astype(BF16)

    for i in range(qg):
        loads[("llm", i)].wait()
        picked = jnp.dot(
            onehot, llm_v[:, i * kc : (i + 1) * kc], preferred_element_type=F32
        ).astype(BF16)
        rows_all[i, 0] = picked[:half]
        rows_all[i, 1] = picked[half:]

    pl.semaphore_wait(barrier, n_grp * n_seq - 1)

    for i in range(qg):
        remote(rows_all.at[i, 1], relay.at[i], xag_sem.at[i], x_peer).start()

    def unless(me, cp):
        @pl.when(jnp.logical_not(me))
        def _():
            cp.start()

        sends.pop()
        sends.append((cp, me))

    def send_rows(src, qq, p):
        cp = remote(src, xin.at[s], xin_sem.at[s], (g, qq * 2 + p))
        me = (qq == q) & (p == c)

        @pl.when(me)
        def _():
            pltpu.make_async_copy(src, xin.at[s], xin_sem.at[s]).start()

        unless(me, cp)

    for i in range(qg):
        send_rows(rows_all.at[i, 0], g * qg + i, 0)

    loads["wf"].wait()
    remote(wout, wo_own, xw_sem.at[0], c_peer).start()
    remote(win, wi_own, xw_sem.at[1], c_peer).start()

    for i in range(qg):
        arrive(relay.at[i], xag_sem.at[i])
        send_rows(relay.at[i], (1 - g) * qg + i, 1)

    fc2_z(1)
    fc2_z(3)
    fc2_near()
    loads["vpre"].wait()
    tile = 64 if pslot % 64 == 0 else 16

    @pl.loop(0, pslot // tile)
    def _(i):
        sl = pl.ds(pl.multiple_of(i * tile, tile), tile)
        v = vpre_v[sl, :].astype(F32)
        sq = jax.nn.sigmoid(1.702 * v)
        act[c, sl, :] = (v * sq).astype(BF16)
        fslope[sl, :] = sq + 1.702 * v * sq * (1.0 - sq)

    remote(act.at[c], act.at[c], xw_sem.at[2], c_peer).start()
    loads["mpre"].wait()
    gslope[...] = gelu_slope(mpre_v[...].astype(F32))

    r = iota((half * n_seq, 1), 0)
    oo = small_div(r, rows)
    rem = r - oo * rows
    src_s = small_div(rem, SLOT)
    slot = rem - src_s * SLOT
    yo = small_div(oo, nz)
    zo = oo - yo * nz
    want = src_s * half + (zo * 2 + yo) * SLOT + slot
    perm = (iota((half * n_seq, half * n_seq), 1) == want).astype(BF16)

    loads["gain"].wait()
    loads["wi"].wait()
    arrive(wi_far, xw_sem.at[1])
    loads["wo"].wait()
    arrive(wo.at[pl.ds(pl.multiple_of((1 - c) * (kc // 2), 16), kc // 2)], xw_sem.at[0])

    first_hand = (g + c + q // qg) % 2 == 0
    for d in range(nz):
        for k in range(4):
            src = zrel(d) * 4 + k
            arrive(xin.at[src], xin_sem.at[src])
            unless(
                jnp.logical_not(first_hand),
                remote(xin.at[src], xin.at[src], xin_sem.at[src], x_peer),
            )
            at = pl.ds(pl.multiple_of(src * half, 8), half)
            xflat[at, :] = xin[src].astype(F32)

    @pl.loop(0, kc // nt)
    def _(t):
        sl = pl.ds(pl.multiple_of(t * nt, nt), nt)
        xperm[:, sl] = jnp.dot(
            perm, xflat[:, sl].astype(BF16), preferred_element_type=F32
        ).astype(BF16)

    hrows = nz * rows

    hh = hid // 2
    order = list(range(nz - 1, -1, -1))

    def part1(yy, hf, out):
        lhs = xperm[pl.ds(pl.multiple_of(yy * hrows, 16), hrows), :]
        got = jnp.dot(lhs, wo[:, hf * hh : (hf + 1) * hh], preferred_element_type=F32)
        for zz in range(nz):
            out[hf, zz] = got[zz * rows : (zz + 1) * rows].astype(out.dtype)

    for hf in range(2):
        part1(1 - y, hf, ys)
        for d in order:
            zz = zrel(d)
            remote(ys.at[hf, zz], ry.at[hf, zz], ry_sem.at[hf, d], y_peer).start()
    for hf in range(2):
        part1(y, hf, own1)
    units = {}

    def over_y(hf, d):
        zz = zrel(d)
        arrive(ry.at[hf, zz], ry_sem.at[hf, d])
        total = own1[hf, zz] + ry[hf, zz].astype(F32)
        if d:
            zs[hf, d] = total.astype(BF16)
            remote(zs.at[hf, d], rz.at[hf, d], rz_sem.at[hf, d], dev(g, zz, y, c)).start()
        else:
            units[hf] = total

    def over_z(hf):
        unit = units[hf]
        for d in order[:-1]:
            arrive(rz.at[hf, d], rz_sem.at[hf, d])
            unit = unit + rz[hf, d].astype(F32)
        slope = gslope[:, hf * hh : (hf + 1) * hh]
        allp[hf, q] = (slope * unit.astype(BF16).astype(F32)).astype(BF16)
        mine = allp.at[hf, q]
        remote(mine, mine, agy_sem.at[hf, 0], y_peer).start()
        for d in order[:-1]:
            remote(mine, mine, agz_sem.at[hf, d], dev(g, zrel(d), y, c)).start()

    for d in order:
        over_y(0, d)
    for d in order:
        over_y(1, d)
    over_z(0)
    over_z(1)
    fc2_y(1)
    near_first = [0] + order[:-1]
    for hf in range(2):
        for d in near_first[1:]:
            qq = zrel(d) * 2 + y
            arrive(allp.at[hf, qq], agz_sem.at[hf, d])
            remote(allp.at[hf, qq], allp.at[hf, qq], agy_sem.at[hf, d], y_peer).start()

    fc2_z(2)
    def columns_of(d):
        zz = zrel(d)
        got = jnp.zeros((2 * rows, cc), F32)
        for hf in range(2):
            arrive(allp.at[hf, zz * 2 + 1 - y], agy_sem.at[hf, d])
            got = got + lax.dot_general(
                allp[hf, pl.ds(zz * 2, 2)].reshape(2 * rows, hh),
                wi[:, hf * hh : (hf + 1) * hh],
                (((1,), (1,)), ((), ())),
                preferred_element_type=F32,
            )
        p2[...] = got
        for e in range(2):
            yo = y + e - 2 * y * e
            far = pl.ds(pl.multiple_of(yo * rows + (1 - g) * half, 8), half)
            near = pl.ds(pl.multiple_of(yo * rows + g * half, 8), half)
            xs[d, e] = p2[far, :].astype(BF16)
            own2[d, e] = p2[near, :].astype(BF16)
        remote(xs.at[d], rx.at[d], rx_sem.at[d], x_peer).start()

    def to_owners(d):
        arrive(rx.at[d], rx_sem.at[d])
        for e in (1, 0):
            yo = y + e - 2 * y * e
            total = (own2[d, e].astype(F32) + rx[d, e].astype(F32)).astype(BF16)
            if d == 0 and e == 0:
                mg[g, q] = total
                remote(mg.at[g, q], mg.at[g, q], mgx_sem.at[q], x_peer).start()
            else:
                a2s[d, e] = total
                remote(
                    a2s.at[d, e], mg.at[g, q], mg_sem.at[q], dev(g, zrel(d), yo, c)
                ).start()

    for k, d in enumerate(near_first):
        columns_of(d)
        if k:
            to_owners(near_first[k - 1])
    fc2_y(3)
    to_owners(near_first[-1])
    def slot_table(gg):
        shape = (phalf, phalf)
        r = iota((phalf, 1), 0)
        src_r = small_div(r, 4 * SLOT)
        place = r - src_r * (4 * SLOT)
        mine = (owners == s) & (shard_of == src_r + gg * (n_seq // 2))
        many = sum_where(mine, jnp.broadcast_to(count, mine.shape))
        wide = sum_where(mine, jnp.broadcast_to(width, mine.shape))
        col = iota(shape, 1)
        comp = small_div(col, half)
        rem = col - comp * half
        src_c = small_div(rem, SLOT)
        slot = rem - src_c * SLOT
        row_in = jnp.zeros(shape, jnp.int32)
        for k in range(1, SLOT):
            row_in = row_in + (slot >= k * wide).astype(jnp.int32)
        col_in = slot - row_in * wide
        upper = comp >> 1
        target = (2 * row_in + upper) * (2 * wide) + 2 * col_in + (comp - 2 * upper)
        return ((src_c == src_r) & (slot < many) & (target == place)).astype(BF16)

    per = vit // cc
    scales = jnp.concatenate([gain_v[k : k + 1, :] for k in range(vit // 128)], axis=1)

    def norm_half(gg, table):
        for qq in range(nq):
            part, spot = qq // per, qq % per
            m4[part * half : (part + 1) * half, spot * cc : (spot + 1) * cc] = mg[
                gg, qq
            ].astype(F32)
        patch_in = jnp.dot(table, m4[...].astype(BF16), preferred_element_type=F32)
        saved = vout_v[pl.ds(pl.multiple_of(gg * phalf, 16), phalf), :].astype(F32)
        pg = norm_backward(patch_in, saved, scales).astype(BF16)
        pgall[c, gg] = pg
        return pg

    loads["vout"].wait()
    far_g = 1 - g
    near_table, far_table = slot_table(g), slot_table(far_g)
    for d in near_first:
        for e in (1, 0) if d else (1,):
            qq = zrel(d) * 2 + y + e - 2 * y * e
            arrive(mg.at[g, qq], mg_sem.at[qq])
            remote(mg.at[g, qq], mg.at[g, qq], mgx_sem.at[qq], x_peer).start()
    fc2_y(2)
    zh = nz // 2
    cuts = [(0, first_lanes), (first_lanes, fhalf - first_lanes)]

    def piece(i, j, side, k):
        lane = pl.multiple_of(side * fhalf + cuts[k][0], 128)
        return pgall.at[i, j, :, pl.ds(lane, cuts[k][1])]

    def to_core(j, k, which):
        at = piece(c, j, 1 - c, k)
        remote(at, at, pgc_sem.at[k, which], c_peer).start()

    pg_out[...] = norm_half(g, near_table)
    for k in range(2):
        to_core(g, k, 0)
    for qq in range(nq):
        arrive(mg.at[far_g, qq], mgx_sem.at[qq])
    norm_half(far_g, far_table)
    for k in range(2):
        to_core(far_g, k, 1)
    fc2_core(0)
    fc2_core(1)
    arrive(act.at[1 - c], xw_sem.at[2])
    quarter = 2 * fw
    acts = act.reshape(2 * pslot, hid)
    sent = 0
    for k in range(2):
        arrive(piece(1 - c, g, c, k), pgc_sem.at[k, 0])
        arrive(piece(1 - c, 1 - g, c, k), pgc_sem.at[k, 1])
        begin, size = cuts[k]
        lhs = jnp.concatenate(
            [piece(i, j, c, k)[...] for i in range(2) for j in range(2)], axis=0
        )
        ready = zh if k else (begin + size) // (2 * quarter)
        for hf in range(2):
            col = slice(hf * hh, (hf + 1) * hh)
            own3[begin : begin + size, col] = lax.dot_general(
                lhs, acts[:, col], (((0,), (0,)), ((), ())), preferred_element_type=F32
            )
            for zz in range(sent, ready):
                base = pl.multiple_of((zz * 2 + 1 - y) * quarter, 16)
                for c2 in range(2):
                    kk = zz * 2 + c2
                    y3s[hf, kk] = own3[pl.ds(base + c2 * fw, fw), col].astype(BF16)
                    remote(
                        y3s.at[hf, kk], ry3.at[hf, kk], ry3_sem.at[hf, kk], y_peer
                    ).start()
        sent = ready
    for zz in range(zh):
        base = pl.multiple_of((zz * 2 + y) * quarter, 16)
        for hf in range(2):
            col = slice(hf * hh, (hf + 1) * hh)
            for c2 in range(2):
                k = zz * 2 + c2
                arrive(ry3.at[hf, k], ry3_sem.at[hf, k])
                total = own3[pl.ds(base + c2 * fw, fw), col] + ry3[hf, k].astype(F32)
                to_z = c * zh + zz
                me = (to_z == z) & (c2 == c)
                z3s[hf, k] = total.astype(BF16)

                @pl.when(me)
                def _():
                    rz3[z, hf] = total.astype(BF16)

                unless(
                    me,
                    remote(
                        z3s.at[hf, k],
                        rz3.at[z, hf],
                        rz3_sem.at[z, hf],
                        dev(g, to_z, y, c2),
                    ),
                )

    fc2_core(3)
    fc2_core(2)
    for d in range(nz):
        for e in range(2):
            yy = y + e - 2 * y * e
            arrive(fc2_block(zrel(d), yy, 1 - c), fc_sem.at[e, d])
    own_pg = jnp.concatenate([pgall[c, 0], pgall[c, 1]], axis=0)
    wfull = wf.reshape(vit, hid)

    @pl.loop(0, hid // nt)
    def _(t):
        sl = pl.ds(pl.multiple_of(t * nt, nt), nt)
        got = jnp.dot(own_pg, wfull[:, sl], preferred_element_type=F32)
        fc1_out[:, sl] = (fslope[:, sl] * got).astype(BF16)

    for hf in range(2):
        total = jnp.zeros((fw, hh), F32)
        for zz in range(nz):

            @pl.when(jnp.logical_not((zz == z) & (c == z // zh)))
            def _():
                arrive(rz3.at[zz, hf], rz3_sem.at[zz, hf])

            total = total + rz3[zz, hf].astype(F32)
        wg_out[:, hf * hh : (hf + 1) * hh] = total

    for item in sends:
        if isinstance(item, tuple):
            cp, me = item

            @pl.when(jnp.logical_not(me))
            def _():
                cp.wait_send()

        else:
            item.wait_send()


def in_hbm(x):
    return pltpu.with_memory_space_constraint(x, pltpu.HBM)


def fused_on_device(
    llm_grad,
    image_grid,
    image_owner,
    row_start,
    merger_pre,
    vit_out,
    vit_pre,
    ln_gain,
    merger_out_w,
    merger_in_w,
    vit_fc2_w,
    *,
    n_grp,
    n_seq,
):
    n_img = image_owner.shape[0]
    tok, feat = llm_grad.shape
    kb, hid = merger_out_w.shape
    cw = merger_in_w.shape[1]
    pslot, _, vit = vit_out.shape
    fw = vit_fc2_w.shape[0]
    rows = merger_pre.shape[0]
    half, phalf = rows // 2, pslot // 2
    nz, nq, kc, cc = n_seq // 4, n_seq // 2, 2 * kb, 2 * cw
    qg = feat // kc
    vmem, anyspace = pltpu.VMEM, pl.BlockSpec(memory_space=pltpu.HBM)
    vspec = pl.BlockSpec(memory_space=pltpu.VMEM)
    dma = pltpu.SemaphoreType.DMA
    scratch = [
        vmem((2, n_img), jnp.int32),
        vmem((1, n_img), jnp.int32),
        vmem((1, n_img), jnp.int32),
        vmem((vit // 128, 128), F32),
        vmem((tok, feat), BF16),
        vmem((rows, hid), BF16),
        vmem((pslot, vit), BF16),
        vmem((pslot, hid), BF16),
        vmem((kc, hid), BF16),
        vmem((cc, hid), BF16),
        vmem((n_seq, fw, hid), BF16),
        vmem((2, pslot, hid), BF16),
        vmem((pslot, hid), F32),
        vmem((rows, hid), F32),
        vmem((qg, 2, half, kc), BF16),
        vmem((qg, half, kc), BF16),
        vmem((n_seq, half, kc), BF16),
        vmem((n_seq * half, kc), F32),
        vmem((n_seq * half, kc), BF16),
        vmem((2, nz, rows, hid // 2), BF16),
        vmem((2, nz, rows, hid // 2), F32),
        vmem((2, nz, rows, hid // 2), BF16),
        vmem((2, nz, rows, hid // 2), BF16),
        vmem((2, nz, rows, hid // 2), BF16),
        vmem((2, nq, rows, hid // 2), BF16),
        vmem((2 * rows, cc), F32),
        vmem((nz, 2, half, cc), BF16),
        vmem((nz, 2, half, cc), BF16),
        vmem((nz, 2, half, cc), BF16),
        vmem((nz, 2, half, cc), BF16),
        vmem((2, nq, half, cc), BF16),
        vmem((phalf, vit), F32),
        vmem((2, 2, phalf, vit), BF16),
        vmem((vit // 2, hid), F32),
        vmem((2, nz, fw, hid // 2), BF16),
        vmem((2, nz, fw, hid // 2), BF16),
        vmem((2, nz, fw, hid // 2), BF16),
        vmem((nz, 2, fw, hid // 2), BF16),
        dma((qg + 10,)),
        dma((320,)),
        dma((3,)),
        dma((qg,)),
        dma((n_seq,)),
        dma((2, nz)),
        dma((2, nz)),
        dma((2, nz)),
        dma((2, nz)),
        dma((nz,)),
        dma((nq,)),
        dma((nz,)),
        dma((nz,)),
        dma((2, nz)),
        dma((nq,)),
        dma((2, 2)),
        dma((2, nz)),
        dma((nz, 2)),
    ]
    pg, fc1, wg = pl.pallas_call(
        functools.partial(fused_kernel, n_grp, n_seq),
        out_shape=(
            jax.ShapeDtypeStruct((phalf, vit), BF16),
            jax.ShapeDtypeStruct((pslot, hid), BF16),
            jax.ShapeDtypeStruct((fw, hid), F32),
        ),
        in_specs=[anyspace] * 11,
        out_specs=(vspec, vspec, vspec),
        scratch_shapes=scratch,
        compiler_params=pltpu.CompilerParams(
            collective_id=0, has_side_effects=True, vmem_limit_bytes=40 * 1024 * 1024
        ),
    )(
        in_hbm(llm_grad),
        in_hbm(image_grid.T),
        in_hbm(image_owner.reshape(1, n_img)),
        in_hbm(row_start.reshape(1, n_img)),
        in_hbm(merger_pre.reshape(rows, hid)),
        in_hbm(vit_out.reshape(pslot, vit)),
        in_hbm(vit_pre.reshape(pslot, hid)),
        in_hbm(ln_gain.reshape(vit // 128, 128)),
        in_hbm(merger_out_w),
        in_hbm(merger_in_w.T),
        in_hbm(vit_fc2_w),
    )
    return pg.reshape(phalf, 1, vit), fc1.reshape(pslot, 1, hid), wg


def solution(mesh):
    n_grp, n_seq = mesh.shape["grp"], mesh.shape["seq"]

    def step(*args):
        llm_grad, merger_pre, vit_out = args[0], args[4], args[5]
        merger_out_w, merger_in_w, vit_fc2_w = args[8], args[9], args[10]
        feat, (kb, hid), cw = llm_grad.shape[1], merger_out_w.shape, merger_in_w.shape[1]
        vit, fw, rows = vit_out.shape[2], vit_fc2_w.shape[0], merger_pre.shape[0]
        fits = (
            n_grp == 2
            and n_seq >= 8
            and n_seq & (n_seq - 1) == 0
            and feat % (2 * kb) == 0
            and kb % 128 == 0
            and hid % 256 == 0
            and (2 * cw) % 128 == 0
            and vit % (2 * cw) == 0
            and vit % 256 == 0
            and fw % 16 == 0
            and rows == n_seq * SLOT
            and rows % 16 == 0
        )
        if fits:
            return fused_on_device(*args, n_grp=n_grp, n_seq=n_seq)
        return on_device(*args)

    return jax.shard_map(
        step,
        mesh=mesh,
        in_specs=(
            P("seq", "grp"),
            P(),
            P(),
            P(),
            P(None, "seq", "grp"),
            P(None, "seq", None),
            P(None, "seq", "grp"),
            P(),
            P("seq", "grp"),
            P("grp", "seq"),
            P("seq", "grp"),
        ),
        out_specs=(P("grp", "seq", None), P(None, "seq", "grp"), P("seq", "grp")),
        check_vma=False,
    )
```
